32 devices in a mesh: gx: 4 (over y, x), gy: 2 (over core), gz: 4 (over z).
Axes of the slice: x: 2, y: 2, z: 4, core: 2. Of those that a mesh axis runs over, the one named last changes fastest.
Arguments:
- right_side: float32 [64, 64, 512], P('gx', 'gy', 'gz'), may hold values from -8 to 8
- diagonal: float32 [64, 64, 512], P('gx', 'gy', 'gz'), may hold values from 0.16 to 6.1
Outputs:
- solution_field: float32 [64, 64, 512], P('gx', 'gy', 'gz')
- residual: float32 [64, 64, 512], P('gx', 'gy', 'gz')
The draws below stay inside these ranges and needn't reach their ends.
All inputs are finite; a program needn't handle non-finite values.
Results may differ from the reference program's by a relative error of at most 0.0003.
Values sent between devices are 32-bit elements; how exact they have to be, the bound alone decides.
A program may use at most 128 MiB of HBM per device.

```python
import math
import jax
import jax.numpy as jnp

ITERS = 2
NX = 64
NY = 64
NZ = 512


def draw_right_side(key, part):
    noise = jax.random.normal(jax.random.fold_in(key, 11), (NX, NY, NZ), jnp.float32)
    values = noise
    return jnp.clip(values, -8.0, 8.0).astype(jnp.float32)


def draw_diagonal(key, part):
    logs = jax.random.uniform(jax.random.fold_in(key, 23), (NX, NY, NZ), jnp.float32, math.log(0.5), math.log(2.0))
    base = jnp.exp(logs)
    place = (jnp.arange(NZ, dtype=jnp.float32) + 0.5) / NZ
    factor = jnp.exp(math.log(3.0) * (2.0 * place - 1.0))
    return (base * factor[None, None, :]).astype(jnp.float32)


def setup_inputs(seed: int = 0) -> dict:
    keys = jax.random.split(jax.random.key(seed), 3)
    right_side = draw_right_side(jax.random.fold_in(keys[2], 71), 0)
    diagonal = draw_diagonal(jax.random.fold_in(keys[2], 71), 0)
    return dict(right_side=right_side, diagonal=diagonal)


def box_sum(padded):
    total = padded[:-2] + padded[1:-1] + padded[2:]
    total = total[:, :-2] + total[:, 1:-1] + total[:, 2:]
    return total[:, :, :-2] + total[:, :, 1:-1] + total[:, :, 2:]


def operate(field, extra):
    return (27.0 + extra) * field - box_sum(jnp.pad(field, 1))


def smooth(rhs, extra, degree, lower):
    upper = 58.0
    theta = (upper + lower) / 2.0
    delta = (upper - lower) / 2.0
    sigma = theta / delta
    rho = 1.0 / sigma
    step = rhs / theta
    total = step
    remain = rhs
    for count in range(degree - 1):
        remain = remain - operate(step, extra)
        rho_next = 1.0 / (2.0 * sigma - rho)
        step = (rho_next * rho) * step + (2.0 * rho_next / delta) * remain
        total = total + step
        rho = rho_next
    return total


def blocks(field):
    a, b, c = field.shape
    return field.reshape(a // 2, 2, b // 2, 2, c // 2, 2)


def restrict(field):
    return 0.5 * blocks(field).sum(axis=(1, 3, 5))


def prolong(field):
    a, b, c = field.shape
    wide = jnp.broadcast_to(field[:, None, :, None, :, None], (a, 2, b, 2, c, 2))
    return wide.reshape(2 * a, 2 * b, 2 * c)


def coarse(r_two, extra_two):
    solved = smooth(r_two, extra_two, 3, 1.0)
    left = r_two - operate(solved, extra_two)
    shift_line = jnp.sum(left, axis=2, keepdims=True) / jnp.sum(1.0 + extra_two, axis=2, keepdims=True)
    return solved + shift_line


def vcycle(r_zero, extra_zero, extra_one, extra_two):
    z_zero = smooth(r_zero, extra_zero, 2, 7.0)
    r_one = restrict(r_zero - operate(z_zero, extra_zero))
    z_one = smooth(r_one, extra_one, 2, 7.0)
    r_two = restrict(r_one - operate(z_one, extra_one))
    z_two = coarse(r_two, extra_two)
    z_one = z_one + prolong(z_two)
    z_one = z_one + smooth(r_one - operate(z_one, extra_one), extra_one, 2, 7.0)
    z_zero = z_zero + prolong(z_one)
    z_zero = z_zero + smooth(r_zero - operate(z_zero, extra_zero), extra_zero, 2, 7.0)
    return z_zero


def reference(right_side, diagonal):
    extra_one = blocks(diagonal).mean(axis=(1, 3, 5))
    extra_two = blocks(extra_one).mean(axis=(1, 3, 5))
    solution_field = jnp.zeros_like(right_side)
    residual = right_side
    direction = jnp.zeros_like(right_side)
    rz_prev = jnp.float32(1.0)
    for step in range(ITERS):
        precond = vcycle(residual, diagonal, extra_one, extra_two)
        rz_now = jnp.sum(residual * precond)
        beta = 0.0 if step == 0 else rz_now / rz_prev
        direction = precond + beta * direction
        image = operate(direction, diagonal)
        alpha = rz_now / jnp.sum(direction * image)
        solution_field = solution_field + alpha * direction
        residual = residual - alpha * image
        rz_prev = rz_now
    return solution_field, residual
```

```python
import functools

import jax
import jax.numpy as jnp
from jax import lax
from jax.experimental import pallas as pl
from jax.experimental.pallas import tpu as pltpu
from jax.sharding import PartitionSpec as P

ITERS = 2
LANES = 128
H = 8
MESH = pl.DeviceIdType.MESH
F32, BF16 = jnp.float32, jnp.bfloat16
UF, UR, U1, UC, UM, UP = 4, 4, 4, 8, 4, 4
OFFSETS = [
    (a, b, c) for a in (-1, 0, 1) for b in (-1, 0, 1) for c in (-1, 0, 1) if (a, b, c) != (0, 0, 0)
]
OFFSETS.sort(key=lambda o: (o[0] == 0, o[2] == 0, o[1] == 0))


def cheb_terms(lower):
    upper = 58.0
    theta = (upper + lower) / 2.0
    delta = (upper - lower) / 2.0
    return theta, delta, theta / delta


def cheb_two(lower):
    theta, delta, sigma = cheb_terms(lower)
    rho = 1.0 / sigma
    rho_next = 1.0 / (2.0 * sigma - rho)
    gain = 2.0 * rho_next / delta
    k2 = gain / theta
    k3 = (1.0 + rho_next * rho) / theta + gain - 27.0 * k2
    return k2, k3


def halves(v):
    high = v.astype(BF16)
    return high, (v - high.astype(F32)).astype(BF16)


def ml(m, v):
    return lax.dot(m[...], jnp.concatenate(halves(v), axis=0), preferred_element_type=F32)


def mr(v, m):
    high, low = halves(v)
    return lax.dot(high, m[...], preferred_element_type=F32) + lax.dot(
        low, m[...], preferred_element_type=F32
    )


def iota(shape, dim):
    return lax.broadcasted_iota(jnp.int32, shape, dim)


def ring(s, rows, lanes):
    s = s + pltpu.roll(s, 1, 0) + pltpu.roll(s, rows - 1, 0)
    return s + pltpu.roll(s, 1, 1) + pltpu.roll(s, lanes - 1, 1)


def box(ref, p):
    s = ref[p - 1] + ref[p] + ref[p + 1]
    return ring(s, *s.shape)


def kernel(
    dims, x_hbm, d_hbm, sol_ref, res_ref,
    x_ref, d_ref, land, edge, face, corner, cland, D, R, Z, T, W, S0,
    land1, edge1, face1, D1, R1a, R1, Z1, T1, send1,
    slots, tile, eslots, etile, rows, row, G, E, Y, Q, M0, M1,
    LyR, RzR, LyP, RzP, LyR2, RzR2, LyP2, RzP2,
    ssem, rsem, gssem, grsem, csem,
):
    GX, GY, GZ = dims
    N = GX * GY * GZ
    nx, ny, nz = x_ref.shape
    n1x, n1y, n1z = nx // 2, ny // 2, nz // 2
    n2x, n2y, n2z = nx // 4, ny // 4, nz // 4
    Y0, Y1 = ny + 2 * H, n1y + 2 * H
    NX2, NY2, NZ2 = GX * n2x, GY * n2y, GZ * n2z
    ix, iy, iz = lax.axis_index("gx"), lax.axis_index("gy"), lax.axis_index("gz")
    me = (ix * GY + iy) * GZ + iz
    k2, k3 = cheb_two(7.0)
    W0 = 2 * LANES

    FAR = (3, 4, 4)
    NEAR = 2
    DEEP = LANES // ny

    def device(n):
        return {"gx": n // (GY * GZ), "gy": (n // GZ) % GY, "gz": n % GZ}

    loads = [
        pltpu.make_async_copy(src, dst, csem.at[i])
        for i, (src, dst) in enumerate(((d_hbm, d_ref), (x_hbm, x_ref)))
    ]
    barrier = pltpu.get_barrier_semaphore()

    def greet(d, _):
        pl.semaphore_signal(barrier, inc=1, device_id=device((me + d) % N), device_id_type=MESH)
        return 0

    lax.fori_loop(1, N, greet, 0)
    for load in loads:
        load.start()

    def cut(o, n, h):
        if o == 0:
            return 0, H, n
        if o > 0:
            return n - h, H - h, h
        return 0, H + n, h

    def there(o, sign):
        ok = None
        for i, g, d in ((ix, GX, o[0]), (iy, GY, o[1]), (iz, GZ, o[2])):
            d = d * sign
            if d:
                t = (i + d >= 0) & (i + d < g)
                ok = t if ok is None else ok & t
        return ok

    def remote(ex, slot, o, src, dst):
        return pltpu.make_async_remote_copy(
            src_ref=src, dst_ref=dst, send_sem=ssem.at[ex, slot], recv_sem=rsem.at[ex, slot],
            device_id={"gx": ix + o[0], "gy": iy + o[1], "gz": iz + o[2]}, device_id_type=MESH,
        )

    def fine(e, core):
        def make(k, far):
            o = a, b, c = OFFSETS[k]
            ys, yd, yn = cut(b, ny, H)
            slot = k
            if c == 0:
                if a == 0:
                    xs, xd, xn = 0, H, nx
                else:
                    lo, hi = (NEAR, FAR[e]) if far else (0, NEAR)
                    xs, xd, xn = (nx - hi, H - hi, hi - lo) if a > 0 else (lo, H + nx + lo, hi - lo)
                    slot = k + far * len(OFFSETS)
                src = core.at[pl.ds(xs, xn), pl.ds(ys, yn)]
                dst = land.at[e, pl.ds(xd, xn), pl.ds(yd, yn)]
            else:
                f, side = (1, 0) if c > 0 else (0, 1)
                if a == 0:
                    src, dst = face.at[e, f, pl.ds(ys, yn)], edge.at[e, side, 1, pl.ds(yd, yn)]
                else:
                    src, dst = corner.at[e, (1 - a) // 2, f], cland.at[e, side, (1 - a) // 2, 1 - b]
            return remote(e, slot, o, src, dst)
        return make

    def level1(ex, e, h):
        def make(k, far):
            o = a, b, c = OFFSETS[k]
            xs, xd, xn = cut(a, n1x, h)
            ys, yd, yn = cut(b, n1y, H)
            if c == 0:
                src = send1.at[e, pl.ds(xs, xn), pl.ds(ys, yn)]
                dst = land1.at[e, pl.ds(xd, xn), pl.ds(yd, yn)]
            else:
                src, dst = face1.at[e, pl.ds(ys, yn)], edge1.at[e, 0 if c > 0 else 1, 1 - a, pl.ds(yd, yn)]
            return remote(ex, k, o, src, dst)
        return make

    FLAT = [k for k, o in enumerate(OFFSETS) if o[2] == 0]
    PACKED = [k for k, o in enumerate(OFFSETS) if o[2] != 0]
    WIDER = [k for k, o in enumerate(OFFSETS) if o[2] == 0 and o[0] != 0]
    sent = []

    def start(makers, ks, far=0):
        for k in ks:
            @pl.when(there(OFFSETS[k], 1))
            def _():
                for make in makers:
                    make(k, far).start()
        sent.append((makers, ks, far))

    def finish(makers, ks, far=0):
        for k in ks:
            @pl.when(there(OFFSETS[k], -1))
            def _():
                for make in makers:
                    make(k, far).wait_recv()

    def drain():
        for makers, ks, far in sent:
            for k in ks:
                @pl.when(there(OFFSETS[k], 1))
                def _():
                    for make in makers:
                        make(k, far).wait_send()

    def ends(k, sender):
        if k == 0:
            return etile, eslots.at[sender]
        if k < 3:
            return tile.at[k - 1], slots.at[k - 1, sender]
        return row.at[k - 3], rows.at[k - 3, sender]

    def gather_copy(k, send_slot, sender, target):
        src, dst = ends(k, sender)
        return pltpu.make_async_remote_copy(
            src_ref=src, dst_ref=dst,
            send_sem=gssem.at[k, send_slot], recv_sem=grsem.at[k, sender],
            device_id=device(target), device_id_type=MESH,
        )

    def gather_start(k):
        def body(d, _):
            gather_copy(k, d, me, (me + d) % N).start()
            return 0
        lax.fori_loop(1, N, body, 0)
        src, dst = ends(k, me)
        dst[...] = src[...]

    def gather_finish(k):
        def body(d, _):
            s = (me + N - d) % N
            gather_copy(k, d, s, s).wait_recv()
            return 0
        lax.fori_loop(1, N, body, 0)

    def gather_drain(k):
        def body(d, _):
            gather_copy(k, d, me, me).wait_send()
            return 0
        lax.fori_loop(1, N, body, 0)

    lane = iota((1, LANES), 1)

    def pack0(e, core):
        first = jnp.zeros((ny, LANES), F32)
        last = jnp.zeros((ny, LANES), F32)
        for x in range(nx):
            v = core[x]
            here = (lane >= H * x) & (lane < H * x + H)
            first = jnp.where(here, pltpu.roll(v, H * x, 1) if x else v, first)
            last = jnp.where(here, pltpu.roll(v, (H * x + H) % LANES, 1) if (H * x + H) % LANES else v, last)
        for f, v in enumerate((first, last)):
            face[e, f] = v
            for i, base in enumerate((nx - DEEP, 0)):
                fold = jnp.zeros((H, LANES), F32)
                for k in range(ny // H):
                    lo = H * DEEP * k
                    shift = (lo - H * base) % LANES
                    part = v[H * k : H * k + H]
                    part = pltpu.roll(part, shift, 1) if shift else part
                    fold = jnp.where((lane >= lo) & (lane < lo + H * DEEP), part, fold)
                corner[e, i, f] = fold

    def unfold(e):
        for side in range(2):
            for i in range(2):
                for k in range(-1, ny // H + 1):
                    v = cland[e, side, i, 0 if k < 0 else 2 if k == ny // H else 1]
                    shift = -H * DEEP * (k % (ny // H)) % LANES
                    edge[e, side, 2 * i, H * k + H : H * k + 2 * H] = pltpu.roll(v, shift, 1) if shift else v

    pl.semaphore_wait(barrier, N - 1)
    for load in loads:
        load.wait()
    both = [fine(0, d_ref), fine(1, x_ref)]
    start(both, FLAT)
    pack0(0, d_ref)
    pack0(1, x_ref)
    start(both, PACKED)
    start(both, WIDER, 1)

    def off0(l):
        return jnp.where(l < 192, l, l - 256)

    def off1(l):
        return jnp.where(l < 96, l, l - 128)

    def pair(fine, coarse):
        return (fine == 2 * coarse) | (fine == 2 * coarse + 1)

    def inside(v, i, n, g):
        v = v + i * n
        return (v >= 0) & (v < g * n)

    def f(cond, value=1.0):
        return jnp.where(cond, F32(value), F32(0.0))

    def twice(m):
        return jnp.concatenate([m, m], axis=1).astype(BF16)

    def near0(z):
        return (z >= -H) & (z < nz + H)

    def near1(z):
        return (z >= -H) & (z < n1z + H)

    yy, zz = iota((Y0, W0), 0) - H, off0(iota((Y0, W0), 1))
    M0[...] = f(inside(yy, iy, ny, GY) & inside(zz, iz, nz, GZ) & near0(zz))
    yy, zz = iota((Y1, LANES), 0) - H, off1(iota((Y1, LANES), 1))
    M1[...] = f(inside(yy, iy, n1y, GY) & inside(zz, iz, n1z, GZ) & near1(zz))
    c, v = iota((Y1, Y0), 0) - H, iota((Y1, Y0), 1) - H
    LyR[...] = twice(f(pair(v, c) & inside(c, iy, n1y, GY), 0.5))
    v, c = iota((Y0, Y1), 0) - H, iota((Y0, Y1), 1) - H
    LyP[...] = twice(f(pair(v, c) & inside(c, iy, n1y, GY)))
    v, c = off0(iota((W0, LANES), 0)), off1(iota((W0, LANES), 1))
    RzR[...] = f(pair(v, c) & inside(c, iz, n1z, GZ) & near0(v)).astype(BF16)
    c, v = off1(iota((LANES, W0), 0)), off0(iota((LANES, W0), 1))
    RzP[...] = f(pair(v, c) & inside(c, iz, n1z, GZ) & near0(v)).astype(BF16)
    c, v = iota((n2y, Y1), 0), iota((n2y, Y1), 1) - H
    LyR2[...] = twice(f(pair(v, c), 0.5))
    v, c = off1(iota((LANES, LANES), 0)), iota((LANES, LANES), 1) % n2z
    RzR2[...] = f(pair(v, c)).astype(BF16)
    v, c = iota((Y1, NY2), 0) - H + iy * n1y, iota((Y1, NY2), 1)
    LyP2[...] = twice(f(pair(v, c)))
    c, v = iota((NZ2, LANES), 0), off1(iota((NZ2, LANES), 1))
    RzP2[...] = f(pair(v + iz * n1z, c) & near1(v)).astype(BF16)

    def xin0(p):
        return f(inside(p - H, ix, nx, GX))

    def xin1(p):
        return f(inside(p - H, ix, n1x, GX))

    def loop(lo, hi, body, group=1):
        count = hi - lo
        while count % group:
            group -= 1

        def step(i, _):
            stores = [body(lo + i * group + k) for k in range(group)]
            for store in stores:
                store()
            return 0
        if count == group:
            step(0, 0)
        else:
            lax.fori_loop(0, count // group, step, 0)

    def put(ref, p, v):
        def store():
            ref[p] = v
        return store

    def merged0(e, core, p, b, sx):
        right = pltpu.roll(edge[e, 1, b], (LANES - H * sx) % LANES, 1)
        left = pltpu.roll(edge[e, 0, b], (2 * LANES - H - H * sx) % LANES, 1)
        return land[e, p], jnp.where(lane < H, right, left)

    def merge0(e, core, emit, far=False):
        near = ((0, H - NEAR, H, DEEP - H), (1, H, H + nx, -H), (2, H + nx, H + nx + NEAR, -H - nx))
        rest = ((0, H - FAR[e], H - NEAR, DEEP - H), (2, H + nx + NEAR, H + nx + FAR[e], -H - nx))
        if not far:
            unfold(e)
            land[e, H : H + nx, H : H + ny] = core[...]
        for b, lo, hi, shift in rest if far else near:
            def body(p, b=b, shift=shift):
                t0, t1 = merged0(e, core, p, b, p + shift)
                ok = M0[...] * xin0(p) > 0.5
                return emit(p, jnp.where(ok, jnp.concatenate([t0, t1], axis=1), 0.0))
            loop(lo, hi, body, UM)

    none = jnp.zeros((2, Y1, LANES), F32)
    R1a[H - 2 : H] = none
    R1a[H + n1x : H + n1x + 2] = none

    def put_d(p, v):
        return put(D, p, v)

    def put_r(p, v):
        return put(R, p, v)

    finish(both, FLAT)
    finish(both, PACKED)
    merge0(0, d_ref, put_d)
    merge0(1, x_ref, put_r)

    def make_d1(p):
        s = D[2 * p - H] + D[2 * p - H + 1]
        return put(D1, p, 0.25 * mr(ml(LyR, s), RzR))

    loop(H - 1, H + n1x + 1, make_d1, 5)

    def pack1(e, src):
        edges = jnp.zeros((n1y, LANES), F32)
        for x in range(n1x):
            v = src[H + x, H : H + n1y]
            send1[e, x] = v
            lo = 2 * H * x
            low = pltpu.roll(v, lo, 1) if lo else v
            up = pltpu.roll(v, (lo + 2 * H - n1z) % LANES, 1) if (lo + 2 * H - n1z) % LANES else v
            edges = jnp.where((lane >= lo) & (lane < lo + H), low, edges)
            edges = jnp.where((lane >= lo + H) & (lane < lo + 2 * H), up, edges)
        face1[e] = edges

    def merge1(e, h, dst, inner=True):
        land1[e, H : H + n1x, H : H + n1y] = send1[e]
        for b, lo, hi, shift in (
            (0, H - h, H, n1x - H), (1, H, H + n1x, -H), (2, H + n1x, H + n1x + h, -H - n1x)
        ):
            if b == 1 and not inner:
                continue

            def body(p, b=b, shift=shift):
                sx = p + shift
                right = pltpu.roll(edge1[e, 1, b], (LANES + n1z - 2 * H * sx) % LANES, 1)
                left = pltpu.roll(edge1[e, 0, b], (2 * LANES - 2 * H - 2 * H * sx) % LANES, 1)
                v = jnp.where(lane < n1z, land1[e, p], jnp.where(lane < n1z + H, right, left))
                return put(dst, p, jnp.where(M1[...] * xin1(p) > 0.5, v, 0.0))
            loop(lo, hi, body, 5)

    pack1(2, D1)
    start([level1(3, 2, 4)], FLAT + PACKED)

    def coarse_tile(s):
        return mr(ml(LyR2, s), RzR2)

    def coarsen(plane):
        total = jnp.zeros((n2y, LANES), F32)
        for x in range(n2x):
            v = coarse_tile(plane(H + 2 * x) + plane(H + 2 * x + 1))
            total = total + jnp.where((lane >= n2z * x) & (lane < n2z * x + n2z), v, 0.0)
        return total

    etile[...] = coarsen(lambda p: D1[p]) * 0.25
    gather_start(0)

    def block(src, q, at):
        shift = (n2z * (q - at)) % LANES
        return pltpu.roll(src, shift, 1) if shift else src

    def along(load, at):
        v = None
        for q in range(LANES // n2z):
            part = block(load(q), q, at)
            v = part if v is None else jnp.where(lane >= n2z * q, part, v)
        return v

    PER = LANES // n2z

    def spread(load, dst, ring):
        def body(a):
            for x in range(n2x):
                for b in range(GY):
                    for t in range(NZ2 // LANES):
                        v = along(lambda q: load((a * GY + b) * GZ + t * PER + q, 0), x)
                        dst[a * n2x + x + 2, n2y * b : n2y * b + n2y, LANES * t : LANES * t + LANES] = v
            return lambda: None
        loop(0, GX, body)
        if not ring:
            return

        def edges(a):
            for b in range(GY):
                for t in range(NZ2 // LANES):
                    for i, p in ((0, a * n2x + 1), (1, (a + 1) * n2x + 2)):
                        v = jnp.concatenate([
                            along(lambda q: load((a * GY + b) * GZ + t * PER + q, 1), i + h) for h in (0, 2)
                        ], axis=0)
                        at = (p, slice(n2y * b, n2y * b + n2y), slice(LANES * t, LANES * t + LANES))
                        dst[at] = dst[at] + v
            return lambda: None
        loop(0, GX, edges)
        zero = jnp.zeros((NY2, NZ2), F32)
        dst[1] = zero
        dst[NX2 + 2] = zero

    rows2, lanes2 = iota((NY2, NZ2), 0), iota((NY2, NZ2), 1)

    def box2(ref, p):
        s = ref[p - 1] + ref[p] + ref[p + 1]
        s = (
            s
            + jnp.where(rows2 > 0, pltpu.roll(s, 1, 0), 0.0)
            + jnp.where(rows2 < NY2 - 1, pltpu.roll(s, NY2 - 1, 0), 0.0)
        )
        return (
            s
            + jnp.where(lanes2 > 0, pltpu.roll(s, 1, 1), 0.0)
            + jnp.where(lanes2 < NZ2 - 1, pltpu.roll(s, NZ2 - 1, 1), 0.0)
        )

    zero2 = jnp.zeros((2, NY2, NZ2), F32)
    for ref in (G, Q, Y):
        ref[0:2] = zero2
        ref[NX2 + 2 : NX2 + 4] = zero2

    def coarse():
        theta, delta, sigma = cheb_terms(1.0)
        rho1 = 1.0 / sigma
        rho2 = 1.0 / (2.0 * sigma - rho1)
        rho3 = 1.0 / (2.0 * sigma - rho2)
        a2, b2 = rho2 * rho1, 2.0 * rho2 / delta
        a3, b3 = rho3 * rho2, 2.0 * rho3 / delta

        def first(p):
            g = G[p]
            remain = g - ((27.0 + E[p]) * g - box2(G, p)) * (1.0 / theta)
            a, b = put(Q, p, (a2 / theta) * g + b2 * remain), put(Y, p, remain)
            return lambda: (a(), b())

        def second(p):
            q, g = Q[p], G[p]
            remain = Y[p] - ((27.0 + E[p]) * q - box2(Q, p))
            return put(Y, p, (1.0 / theta) * g + (1.0 + a3) * q + b3 * remain)

        def third(p):
            y = Y[p]
            left = G[p] - ((27.0 + E[p]) * y - box2(Y, p))
            shift = jnp.sum(left, axis=1, keepdims=True) / jnp.sum(1.0 + E[p], axis=1, keepdims=True)
            return put(Q, p, y + shift)

        for body in (first, second, third):
            loop(2, NX2 + 2, body, UC)

    def smooth1(ref, p):
        return ref[p] * (k3 - k2 * D1[p]) + k2 * box(ref, p)

    def precondition(it):
        ex = 4 + it

        def down0(p):
            return put(Z, p, (M0[...] * xin0(p)) * (R[p] * (k3 - k2 * D[p]) + k2 * box(R, p)))

        loop(H - 1, H + nx + 1, down0, 6)

        def rest0(p):
            return R[p] - ((27.0 + D[p]) * Z[p] - box(Z, p))

        def down1(p):
            s = rest0(2 * p - H) + rest0(2 * p - H + 1)
            return put(R1a, p, mr(ml(LyR, s), RzR))

        loop(H, H + n1x, down1, UR)

        pack1(it, R1a)
        fine1 = [level1(ex, it, 5)]
        start(fine1, FLAT + PACKED)

        Z1[H - 3 : H - 1] = none
        Z1[H + n1x + 1 : H + n1x + 3] = none

        def z1a(p):
            return put(Z1, p, (M1[...] * xin1(p)) * smooth1(R1a, p))

        loop(H - 1, H + n1x + 1, z1a, 5)

        def rest1(p):
            return R1a[p] - ((27.0 + D1[p]) * Z1[p] - box(Z1, p))

        tile[it, 0:n2y] = coarsen(rest1)
        low = coarse_tile(box(Z1, H - 2) + rest1(H - 1))
        high = coarse_tile(rest1(H + n1x) + box(Z1, H + n1x + 1))
        low, high = (jnp.where(lane < 2 * n2z, v, pltpu.roll(v, n2y // 2, 0)) for v in (low, high))
        ring2 = jnp.where(lane // n2z % 2 == 0, low, high)
        tile[it, n2y : n2y + n2y // 2] = ring2[0 : n2y // 2]
        gather_start(1 + it)

        far(it)
        for lo, hi in ((H - 3, H - 1), (H + nx + 1, H + nx + 3)):
            loop(lo, hi, down0, 2)

        finish(fine1, FLAT + PACKED)
        merge1(it, 5, R1)
        if it == 0:
            finish([level1(3, 2, 4)], FLAT + PACKED)
            merge1(2, 4, D1, False)

        def z1b(p):
            return put(Z1, p, (M1[...] * xin1(p)) * smooth1(R1, p))

        loop(H - 4, H + n1x + 4, z1b, U1)

        if it == 0:
            gather_finish(0)
            spread(lambda n, r: eslots[n], E, False)
        gather_finish(1 + it)
        spread(lambda n, r: slots[it, n, n2y:] if r else slots[it, n, 0:n2y], G, True)
        coarse()

        def up1(q):
            v = mr(ml(LyP2, Q[ix * n2x + q]), RzP2)
            p = H - 4 + 2 * q
            a, b = put(Z1, p, Z1[p] + v), put(Z1, p + 1, Z1[p + 1] + v)
            return lambda: (a(), b())

        loop(0, n2x + 4, up1, 4)

        def t1(p):
            return put(T1, p, (M1[...] * xin1(p)) * (R1[p] - ((27.0 + D1[p]) * Z1[p] - box(Z1, p))))

        loop(H - 3, H + n1x + 3, t1, U1)

        def z1c(p):
            return put(Z1, p, Z1[p] + (M1[...] * xin1(p)) * smooth1(T1, p))

        loop(H - 2, H + n1x + 2, z1c, U1)

        def up0(p):
            v = mr(ml(LyP, Z1[p]), RzP)
            q = 2 * p - H
            a, b = put(Z, q, Z[q] + v), put(Z, q + 1, Z[q + 1] + v)
            return lambda: (a(), b())

        loop(H - 2, H + n1x + 2, up0, UR)

        def t0(p):
            return put(T, p, (M0[...] * xin0(p)) * rest0(p))

        loop(H - 2, H + nx + 2, t0, UF)

        def z0(p):
            return put(Z, p, Z[p] + (M0[...] * xin0(p)) * (T[p] * (k3 - k2 * D[p]) + k2 * box(T, p)))

        loop(H - 1, H + nx + 1, z0, UF)

    core = (slice(H, H + ny), slice(0, nz))

    def products(it):
        def one(x, carry):
            p = x + H
            z = Z[p]
            w = ((27.0 + D[p]) * z - box(Z, p))[core[0], core[1]]
            z = z[core[0], core[1]]
            W[it, x] = w
            S0[it, x] = z
            r = R[p, core[0], core[1]]
            out = [carry[0] + r * z, carry[1] + z * w]
            if it:
                out.append(carry[2] + z * W[0, x])
            return tuple(out)

        def body(i, carry):
            for k in range(UP):
                carry = one(i * UP + k, carry)
            return carry

        init = tuple(jnp.zeros((ny, nz), F32) for _ in range(3 if it else 2))
        sums = lax.fori_loop(0, nx // UP, body, init)
        v = jnp.zeros((1, LANES), F32)
        for i, s in enumerate(sums):
            s = jnp.sum(jnp.sum(s, axis=0, keepdims=True), axis=1, keepdims=True)
            v = jnp.where(lane == i, s, v)
        row[it] = v
        gather_start(3 + it)

    def total(k):
        gather_finish(k)

        def body(n, acc):
            return acc + rows[k - 3, n]

        acc = lax.fori_loop(0, N, body, jnp.zeros((1, LANES), F32))
        return acc[:, 0:1], acc[:, 1:2], acc[:, 2:3]

    def far(it):
        if it == 0:
            finish(both, WIDER, 1)
            merge0(0, d_ref, put_d, True)
            merge0(1, x_ref, put_r, True)
        else:
            finish(image, WIDER, 1)
            merge0(2, W.at[0], put_image, True)

    precondition(0)
    products(0)
    image = [fine(2, W.at[0])]
    start(image, FLAT)
    pack0(2, W.at[0])
    start(image, PACKED)
    start(image, WIDER, 1)
    rz0, curve0, _ = total(3)
    alpha0 = rz0 / curve0
    finish(image, FLAT)
    finish(image, PACKED)

    def put_image(p, v):
        return put(R, p, R[p] - alpha0 * v)

    merge0(2, W.at[0], put_image)
    precondition(1)
    products(1)
    rz1, zw, zq = total(4)
    beta = rz1 / rz0
    curve = zw + 2.0 * beta * zq + beta * beta * curve0
    alpha = rz1 / curve

    def last(x):
        z = S0[0, x]
        sol_ref[x] = alpha0 * z + alpha * (S0[1, x] + beta * z)
        res_ref[x] = R[x + H, core[0], core[1]] - alpha * (W[1, x] + beta * W[0, x])
        return lambda: None

    loop(0, nx, last, 4)
    drain()
    for k in range(5):
        gather_drain(k)


def solution(mesh):
    dims = (mesh.shape["gx"], mesh.shape["gy"], mesh.shape["gz"])
    N = dims[0] * dims[1] * dims[2]

    def local(right_side, diagonal):
        nx, ny, nz = right_side.shape
        assert nz == LANES and nx * H == LANES and (nx // 4) * (nz // 4) == LANES and ny == 32
        n1x, n1y, n2y = nx // 2, ny // 2, ny // 4
        X0, Y0, X1, Y1 = nx + 2 * H, ny + 2 * H, n1x + 2 * H, n1y + 2 * H
        NX2, NY2, NZ2 = dims[0] * nx // 4, dims[1] * n2y, dims[2] * nz // 4
        W0 = 2 * LANES
        vm = lambda *s: pltpu.VMEM(s, F32)
        vb = lambda *s: pltpu.VMEM(s, BF16)
        dma = pltpu.SemaphoreType.DMA
        scratch = [
            vm(nx, ny, nz), vm(nx, ny, nz),
            vm(3, X0, Y0, LANES), vm(3, 2, 3, Y0, LANES), vm(3, 2, ny, LANES),
            vm(3, 2, 2, H, LANES), vm(3, 2, 2, 3, H, LANES),
            vm(X0, Y0, W0), vm(X0, Y0, W0), vm(X0, Y0, W0), vm(X0, Y0, W0),
            vm(2, nx, ny, nz), vm(2, nx, ny, nz),
            vm(3, X1, Y1, LANES), vm(3, 2, 3, Y1, LANES), vm(3, n1y, LANES),
            vm(X1, Y1, LANES), vm(X1, Y1, LANES), vm(X1, Y1, LANES), vm(X1, Y1, LANES), vm(X1, Y1, LANES),
            vm(3, n1x, n1y, LANES),
            vm(2, N, n2y * 3 // 2, LANES), vm(2, n2y * 3 // 2, LANES), vm(N, n2y, LANES), vm(n2y, LANES), vm(2, N, 1, LANES), vm(2, 1, LANES),
            vm(NX2 + 4, NY2, NZ2), vm(NX2 + 4, NY2, NZ2), vm(NX2 + 4, NY2, NZ2), vm(NX2 + 4, NY2, NZ2),
            vm(Y0, W0), vm(Y1, LANES),
            vb(Y1, 2 * Y0), vb(W0, LANES), vb(Y0, 2 * Y1), vb(LANES, W0),
            vb(n2y, 2 * Y1), vb(LANES, LANES), vb(Y1, 2 * NY2), vb(NZ2, LANES),
            dma((6, 52)), dma((6, 52)), dma((5, N)), dma((5, N)), dma((2,)),
        ]
        shape = jax.ShapeDtypeStruct(right_side.shape, F32)
        return pl.pallas_call(
            functools.partial(kernel, dims),
            out_shape=(shape, shape),
            in_specs=[pl.BlockSpec(memory_space=pl.ANY)] * 2,
            out_specs=[pl.BlockSpec(memory_space=pltpu.VMEM)] * 2,
            scratch_shapes=scratch,
            compiler_params=pltpu.CompilerParams(collective_id=0, has_side_effects=True),
        )(right_side, diagonal)

    placed = (P("gx", "gy", "gz"), P("gx", "gy", "gz"))
    return jax.shard_map(local, mesh=mesh, in_specs=placed, out_specs=placed, check_vma=False)
```

```python
import functools
import math

import jax
import jax.numpy as jnp
from jax import lax
from jax.experimental import pallas as pl
from jax.experimental.pallas import tpu as pltpu
from jax.sharding import PartitionSpec as P

ITERS = 2
LANES = 128
H = 8
MESH = pl.DeviceIdType.MESH
F32, BF16 = jnp.float32, jnp.bfloat16
UF, UR, U1, UC, UM, UP = 4, 4, 4, 8, 4, 4
OFFSETS = [
    (a, b, c) for a in (-1, 0, 1) for b in (-1, 0, 1) for c in (-1, 0, 1) if (a, b, c) != (0, 0, 0)
]
OFFSETS.sort(key=lambda o: (o[0] == 0, o[2] == 0, o[1] == 0))


def cheb_terms(lower):
    upper = 58.0
    theta = (upper + lower) / 2.0
    delta = (upper - lower) / 2.0
    return theta, delta, theta / delta


def cheb_two(lower):
    theta, delta, sigma = cheb_terms(lower)
    rho = 1.0 / sigma
    rho_next = 1.0 / (2.0 * sigma - rho)
    gain = 2.0 * rho_next / delta
    k2 = gain / theta
    k3 = (1.0 + rho_next * rho) / theta + gain - 27.0 * k2
    return k2, k3


def halves(v):
    high = v.astype(BF16)
    return high, (v - high.astype(F32)).astype(BF16)


def ml(m, v):
    return lax.dot(m[...], jnp.concatenate(halves(v), axis=0), preferred_element_type=F32)


def mr(v, m):
    high, low = halves(v)
    return lax.dot(high, m[...], preferred_element_type=F32) + lax.dot(
        low, m[...], preferred_element_type=F32
    )


def iota(shape, dim):
    return lax.broadcasted_iota(jnp.int32, shape, dim)


def ring(s, rows, lanes):
    s = s + pltpu.roll(s, 1, 0) + pltpu.roll(s, rows - 1, 0)
    return s + pltpu.roll(s, 1, 1) + pltpu.roll(s, lanes - 1, 1)


def box(ref, p):
    s = ref[p - 1] + ref[p] + ref[p + 1]
    return ring(s, *s.shape)


def kernel(
    dims, x_hbm, d_hbm, sol_ref, res_ref,
    x_ref, d_ref, land, edge, face, corner, cland, D, R, Z, T, W, S0,
    land1, edge1, face1, D1, R1a, R1, Z1, T1, send1,
    slots, tile, eslots, etile, rows, row, G, E, Y, Q, M0, M1,
    LyR, RzR, LyP, RzP, LyR2, RzR2, LyP2, RzP2,
    spare, ssem, rsem, gssem, grsem, csem,
):
    GX, GY, GZ = dims
    N = GX * GY * GZ
    nx, ny, nz = x_ref.shape
    n1x, n1y, n1z = nx // 2, ny // 2, nz // 2
    n2x, n2y, n2z = nx // 4, ny // 4, nz // 4
    Y0, Y1 = ny + 2 * H, n1y + 2 * H
    NX2, NY2, NZ2 = GX * n2x, GY * n2y, GZ * n2z
    ix, iy, iz = lax.axis_index("gx"), lax.axis_index("gy"), lax.axis_index("gz")
    me = (ix * GY + iy) * GZ + iz
    k2, k3 = cheb_two(7.0)
    W0 = 2 * LANES

    FAR = (3, 4, 4)
    NEAR = 2
    DEEP = LANES // ny

    def device(n):
        return {"gx": n // (GY * GZ), "gy": (n // GZ) % GY, "gz": n % GZ}

    loads = [
        pltpu.make_async_copy(src, dst, csem.at[i])
        for i, (src, dst) in enumerate(((d_hbm, d_ref), (x_hbm, x_ref)))
    ]
    barrier = pltpu.get_barrier_semaphore()

    def greet(d, _):
        pl.semaphore_signal(barrier, inc=1, device_id=device((me + d) % N), device_id_type=MESH)
        return 0

    lax.fori_loop(1, N, greet, 0)
    for load in loads:
        load.start()

    def cut(o, n, h):
        if o == 0:
            return 0, H, n
        if o > 0:
            return n - h, H - h, h
        return 0, H + n, h

    def there(o, sign):
        ok = None
        for i, g, d in ((ix, GX, o[0]), (iy, GY, o[1]), (iz, GZ, o[2])):
            d = d * sign
            if d:
                t = (i + d >= 0) & (i + d < g)
                ok = t if ok is None else ok & t
        return ok

    def remote(ex, o, src, dst):
        return pltpu.make_async_remote_copy(
            src_ref=src, dst_ref=dst, send_sem=ssem.at[ex], recv_sem=rsem.at[ex],
            device_id={"gx": ix + o[0], "gy": iy + o[1], "gz": iz + o[2]}, device_id_type=MESH,
        )

    def fine(ex, e, core):
        def make(k, far):
            o = a, b, c = OFFSETS[k]
            ys, yd, yn = cut(b, ny, H)
            if c == 0:
                if a == 0:
                    xs, xd, xn = 0, H, nx
                else:
                    lo, hi = (NEAR, FAR[e]) if far else (0, NEAR)
                    xs, xd, xn = (nx - hi, H - hi, hi - lo) if a > 0 else (lo, H + nx + lo, hi - lo)
                src = core.at[pl.ds(xs, xn), pl.ds(ys, yn)]
                dst = land.at[e, pl.ds(xd, xn), pl.ds(yd, yn)]
            else:
                f, side = (1, 0) if c > 0 else (0, 1)
                if a == 0:
                    src, dst = face.at[e, f, pl.ds(ys, yn)], edge.at[e, side, 1, pl.ds(yd, yn)]
                else:
                    src, dst = corner.at[e, (1 - a) // 2, f], cland.at[e, side, (1 - a) // 2, 1 - b]
            return ex + far, o, src, dst
        return make

    def level1(ex, e, h):
        def make(k, far):
            o = a, b, c = OFFSETS[k]
            xs, xd, xn = cut(a, n1x, h)
            ys, yd, yn = cut(b, n1y, H)
            if c == 0:
                src = send1.at[e, pl.ds(xs, xn), pl.ds(ys, yn)]
                dst = land1.at[e, pl.ds(xd, xn), pl.ds(yd, yn)]
            else:
                src, dst = face1.at[e, pl.ds(ys, yn)], edge1.at[e, 0 if c > 0 else 1, 1 - a, pl.ds(yd, yn)]
            return ex, o, src, dst
        return make

    FLAT = [k for k, o in enumerate(OFFSETS) if o[2] == 0]
    PACKED = [k for k, o in enumerate(OFFSETS) if o[2] != 0]
    WIDER = [k for k, o in enumerate(OFFSETS) if o[2] == 0 and o[0] != 0]
    sent = []

    def start(makers, ks, far=0):
        for k in ks:
            @pl.when(there(OFFSETS[k], 1))
            def _():
                for make in makers:
                    remote(*make(k, far)).start()

    def counts(i, g):
        if g < 3:
            return [(g - 1, None)]
        outer = (i == 0) | (i == g - 1)
        return [(1, outer), (2, jnp.logical_not(outer))]

    def settle(makers, ks, far, received):
        for cx, px in counts(ix, GX):
            for cy, py in counts(iy, GY):
                for cz, pz in counts(iz, GZ):
                    n = 0
                    for k in ks:
                        a, b, c = OFFSETS[k]
                        if min(a, b, c) >= 0:
                            times = (cx if a else 1) * (cy if b else 1) * (cz if c else 1)
                            for make in makers:
                                n += times * math.prod(make(k, far)[2].shape) // (H * LANES)
                    if n == 0:
                        continue
                    some = spare.at[pl.ds(0, n)]
                    copy = remote(makers[0](0, far)[0], (0, 0, 1), some, some)
                    wait = copy.wait_recv if received else copy.wait_send
                    ok = [p for p in (px, py, pz) if p is not None]
                    if ok:
                        pl.when(functools.reduce(jnp.logical_and, ok))(wait)
                    else:
                        wait()

    def finish(makers, ks, far=0):
        settle(makers, ks, far, True)
        sent.append((makers, ks, far))

    def drain():
        for makers, ks, far in sent:
            settle(makers, ks, far, False)

    def ends(k, sender):
        if k == 0:
            return etile, eslots.at[sender]
        if k < 3:
            return tile.at[k - 1], slots.at[k - 1, sender]
        return row.at[k - 3], rows.at[k - 3, sender]

    def gather_start(k):
        src, dst = ends(k, me)

        def body(d, _):
            pltpu.make_async_remote_copy(
                src_ref=src, dst_ref=dst, send_sem=gssem.at[k], recv_sem=grsem.at[k],
                device_id=device((me + d) % N), device_id_type=MESH,
            ).start()
            return 0
        lax.fori_loop(1, N, body, 0)
        dst[...] = src[...]

    def everyone(k):
        some = pl.ds(0, N - 1)
        ref = eslots.at[some] if k == 0 else slots.at[k - 1, some] if k < 3 else rows.at[k - 3, some]
        return pltpu.make_async_remote_copy(
            src_ref=ref, dst_ref=ref, send_sem=gssem.at[k], recv_sem=grsem.at[k],
            device_id=device((me + 1) % N), device_id_type=MESH,
        )

    def gather_finish(k):
        everyone(k).wait_recv()

    def gather_drain(k):
        everyone(k).wait_send()

    lane = iota((1, LANES), 1)

    def pack0(e, core):
        first = jnp.zeros((ny, LANES), F32)
        last = jnp.zeros((ny, LANES), F32)
        for x in range(nx):
            v = core[x]
            here = (lane >= H * x) & (lane < H * x + H)
            first = jnp.where(here, pltpu.roll(v, H * x, 1) if x else v, first)
            last = jnp.where(here, pltpu.roll(v, (H * x + H) % LANES, 1) if (H * x + H) % LANES else v, last)
        for f, v in enumerate((first, last)):
            face[e, f] = v
            for i, base in enumerate((nx - DEEP, 0)):
                fold = jnp.zeros((H, LANES), F32)
                for k in range(ny // H):
                    lo = H * DEEP * k
                    shift = (lo - H * base) % LANES
                    part = v[H * k : H * k + H]
                    part = pltpu.roll(part, shift, 1) if shift else part
                    fold = jnp.where((lane >= lo) & (lane < lo + H * DEEP), part, fold)
                corner[e, i, f] = fold

    def unfold(e):
        for side in range(2):
            for i in range(2):
                for k in range(-1, ny // H + 1):
                    v = cland[e, side, i, 0 if k < 0 else 2 if k == ny // H else 1]
                    shift = -H * DEEP * (k % (ny // H)) % LANES
                    edge[e, side, 2 * i, H * k + H : H * k + 2 * H] = pltpu.roll(v, shift, 1) if shift else v

    pl.semaphore_wait(barrier, N - 1)
    for load in loads:
        load.wait()
    both = [fine(0, 0, d_ref), fine(0, 1, x_ref)]
    start(both, FLAT)
    pack0(0, d_ref)
    pack0(1, x_ref)
    start(both, PACKED)
    start(both, WIDER, 1)

    def off0(l):
        return jnp.where(l < 192, l, l - 256)

    def off1(l):
        return jnp.where(l < 96, l, l - 128)

    def pair(fine, coarse):
        return (fine == 2 * coarse) | (fine == 2 * coarse + 1)

    def inside(v, i, n, g):
        v = v + i * n
        return (v >= 0) & (v < g * n)

    def f(cond, value=1.0):
        return jnp.where(cond, F32(value), F32(0.0))

    def twice(m):
        return jnp.concatenate([m, m], axis=1).astype(BF16)

    def near0(z):
        return (z >= -H) & (z < nz + H)

    def near1(z):
        return (z >= -H) & (z < n1z + H)

    yy, zz = iota((Y0, W0), 0) - H, off0(iota((Y0, W0), 1))
    M0[...] = f(inside(yy, iy, ny, GY) & inside(zz, iz, nz, GZ) & near0(zz))
    yy, zz = iota((Y1, LANES), 0) - H, off1(iota((Y1, LANES), 1))
    M1[...] = f(inside(yy, iy, n1y, GY) & inside(zz, iz, n1z, GZ) & near1(zz))
    c, v = iota((Y1, Y0), 0) - H, iota((Y1, Y0), 1) - H
    LyR[...] = twice(f(pair(v, c) & inside(c, iy, n1y, GY), 0.5))
    v, c = iota((Y0, Y1), 0) - H, iota((Y0, Y1), 1) - H
    LyP[...] = twice(f(pair(v, c) & inside(c, iy, n1y, GY)))
    v, c = off0(iota((W0, LANES), 0)), off1(iota((W0, LANES), 1))
    RzR[...] = f(pair(v, c) & inside(c, iz, n1z, GZ) & near0(v)).astype(BF16)
    c, v = off1(iota((LANES, W0), 0)), off0(iota((LANES, W0), 1))
    RzP[...] = f(pair(v, c) & inside(c, iz, n1z, GZ) & near0(v)).astype(BF16)
    c, v = iota((n2y, Y1), 0), iota((n2y, Y1), 1) - H
    LyR2[...] = twice(f(pair(v, c), 0.5))
    v, c = off1(iota((LANES, LANES), 0)), iota((LANES, LANES), 1) % n2z
    RzR2[...] = f(pair(v, c)).astype(BF16)
    v, c = iota((Y1, NY2), 0) - H + iy * n1y, iota((Y1, NY2), 1)
    LyP2[...] = twice(f(pair(v, c)))
    c, v = iota((NZ2, LANES), 0), off1(iota((NZ2, LANES), 1))
    RzP2[...] = f(pair(v + iz * n1z, c) & near1(v)).astype(BF16)

    def xin0(p):
        return f(inside(p - H, ix, nx, GX))

    def xin1(p):
        return f(inside(p - H, ix, n1x, GX))

    def loop(lo, hi, body, group=1):
        count = hi - lo
        while count % group:
            group -= 1

        def step(i, _):
            stores = [body(lo + i * group + k) for k in range(group)]
            for store in stores:
                store()
            return 0
        if count == group:
            step(0, 0)
        else:
            lax.fori_loop(0, count // group, step, 0)

    def put(ref, p, v):
        def store():
            ref[p] = v
        return store

    def merged0(e, core, p, b, sx):
        right = pltpu.roll(edge[e, 1, b], (LANES - H * sx) % LANES, 1)
        left = pltpu.roll(edge[e, 0, b], (2 * LANES - H - H * sx) % LANES, 1)
        return land[e, p], jnp.where(lane < H, right, left)

    def merge0(e, core, emit, far=False):
        near = ((0, H - NEAR, H, DEEP - H), (1, H, H + nx, -H), (2, H + nx, H + nx + NEAR, -H - nx))
        rest = ((0, H - FAR[e], H - NEAR, DEEP - H), (2, H + nx + NEAR, H + nx + FAR[e], -H - nx))
        if not far:
            unfold(e)
            land[e, H : H + nx, H : H + ny] = core[...]
        for b, lo, hi, shift in rest if far else near:
            def body(p, b=b, shift=shift):
                t0, t1 = merged0(e, core, p, b, p + shift)
                ok = M0[...] * xin0(p) > 0.5
                return emit(p, jnp.where(ok, jnp.concatenate([t0, t1], axis=1), 0.0))
            loop(lo, hi, body, UM)

    none = jnp.zeros((2, Y1, LANES), F32)
    R1a[H - 2 : H] = none
    R1a[H + n1x : H + n1x + 2] = none

    def put_d(p, v):
        return put(D, p, v)

    def put_r(p, v):
        return put(R, p, v)

    finish(both, FLAT + PACKED)
    merge0(0, d_ref, put_d)
    merge0(1, x_ref, put_r)

    def make_d1(p):
        s = D[2 * p - H] + D[2 * p - H + 1]
        return put(D1, p, 0.25 * mr(ml(LyR, s), RzR))

    loop(H - 1, H + n1x + 1, make_d1, 5)

    def pack1(e, src):
        edges = jnp.zeros((n1y, LANES), F32)
        for x in range(n1x):
            v = src[H + x, H : H + n1y]
            send1[e, x] = v
            lo = 2 * H * x
            low = pltpu.roll(v, lo, 1) if lo else v
            up = pltpu.roll(v, (lo + 2 * H - n1z) % LANES, 1) if (lo + 2 * H - n1z) % LANES else v
            edges = jnp.where((lane >= lo) & (lane < lo + H), low, edges)
            edges = jnp.where((lane >= lo + H) & (lane < lo + 2 * H), up, edges)
        face1[e] = edges

    def merge1(e, h, dst, inner=True):
        land1[e, H : H + n1x, H : H + n1y] = send1[e]
        for b, lo, hi, shift in (
            (0, H - h, H, n1x - H), (1, H, H + n1x, -H), (2, H + n1x, H + n1x + h, -H - n1x)
        ):
            if b == 1 and not inner:
                continue

            def body(p, b=b, shift=shift):
                sx = p + shift
                right = pltpu.roll(edge1[e, 1, b], (LANES + n1z - 2 * H * sx) % LANES, 1)
                left = pltpu.roll(edge1[e, 0, b], (2 * LANES - 2 * H - 2 * H * sx) % LANES, 1)
                v = jnp.where(lane < n1z, land1[e, p], jnp.where(lane < n1z + H, right, left))
                return put(dst, p, jnp.where(M1[...] * xin1(p) > 0.5, v, 0.0))
            loop(lo, hi, body, 5)

    pack1(2, D1)
    start([level1(6, 2, 4)], FLAT + PACKED)

    def coarse_tile(s):
        return mr(ml(LyR2, s), RzR2)

    def coarsen(plane):
        total = jnp.zeros((n2y, LANES), F32)
        for x in range(n2x):
            v = coarse_tile(plane(H + 2 * x) + plane(H + 2 * x + 1))
            total = total + jnp.where((lane >= n2z * x) & (lane < n2z * x + n2z), v, 0.0)
        return total

    etile[...] = coarsen(lambda p: D1[p]) * 0.25
    gather_start(0)

    def block(src, q, at):
        shift = (n2z * (q - at)) % LANES
        return pltpu.roll(src, shift, 1) if shift else src

    def along(load, at):
        v = None
        for q in range(LANES // n2z):
            part = block(load(q), q, at)
            v = part if v is None else jnp.where(lane >= n2z * q, part, v)
        return v

    PER = LANES // n2z

    def spread(load, dst, ring):
        def body(a):
            for x in range(n2x):
                for b in range(GY):
                    for t in range(NZ2 // LANES):
                        v = along(lambda q: load((a * GY + b) * GZ + t * PER + q, 0), x)
                        dst[a * n2x + x + 2, n2y * b : n2y * b + n2y, LANES * t : LANES * t + LANES] = v
            return lambda: None
        loop(0, GX, body)
        if not ring:
            return

        def edges(a):
            for b in range(GY):
                for t in range(NZ2 // LANES):
                    for i, p in ((0, a * n2x + 1), (1, (a + 1) * n2x + 2)):
                        v = jnp.concatenate([
                            along(lambda q: load((a * GY + b) * GZ + t * PER + q, 1), i + h) for h in (0, 2)
                        ], axis=0)
                        at = (p, slice(n2y * b, n2y * b + n2y), slice(LANES * t, LANES * t + LANES))
                        dst[at] = dst[at] + v
            return lambda: None
        loop(0, GX, edges)
        zero = jnp.zeros((NY2, NZ2), F32)
        dst[1] = zero
        dst[NX2 + 2] = zero

    rows2, lanes2 = iota((NY2, NZ2), 0), iota((NY2, NZ2), 1)

    def box2(ref, p):
        s = ref[p - 1] + ref[p] + ref[p + 1]
        s = (
            s
            + jnp.where(rows2 > 0, pltpu.roll(s, 1, 0), 0.0)
            + jnp.where(rows2 < NY2 - 1, pltpu.roll(s, NY2 - 1, 0), 0.0)
        )
        return (
            s
            + jnp.where(lanes2 > 0, pltpu.roll(s, 1, 1), 0.0)
            + jnp.where(lanes2 < NZ2 - 1, pltpu.roll(s, NZ2 - 1, 1), 0.0)
        )

    zero2 = jnp.zeros((2, NY2, NZ2), F32)
    for ref in (G, Q, Y):
        ref[0:2] = zero2
        ref[NX2 + 2 : NX2 + 4] = zero2

    def coarse():
        theta, delta, sigma = cheb_terms(1.0)
        rho1 = 1.0 / sigma
        rho2 = 1.0 / (2.0 * sigma - rho1)
        rho3 = 1.0 / (2.0 * sigma - rho2)
        a2, b2 = rho2 * rho1, 2.0 * rho2 / delta
        a3, b3 = rho3 * rho2, 2.0 * rho3 / delta

        def first(p):
            g = G[p]
            remain = g - ((27.0 + E[p]) * g - box2(G, p)) * (1.0 / theta)
            a, b = put(Q, p, (a2 / theta) * g + b2 * remain), put(Y, p, remain)
            return lambda: (a(), b())

        def second(p):
            q, g = Q[p], G[p]
            remain = Y[p] - ((27.0 + E[p]) * q - box2(Q, p))
            return put(Y, p, (1.0 / theta) * g + (1.0 + a3) * q + b3 * remain)

        def third(p):
            y = Y[p]
            left = G[p] - ((27.0 + E[p]) * y - box2(Y, p))
            shift = jnp.sum(left, axis=1, keepdims=True) / jnp.sum(1.0 + E[p], axis=1, keepdims=True)
            return put(Q, p, y + shift)

        for body in (first, second, third):
            loop(2, NX2 + 2, body, UC)

    def smooth1(ref, p):
        return ref[p] * (k3 - k2 * D1[p]) + k2 * box(ref, p)

    def precondition(it):
        ex = 4 + it

        def down0(p):
            return put(Z, p, (M0[...] * xin0(p)) * (R[p] * (k3 - k2 * D[p]) + k2 * box(R, p)))

        loop(H - 1, H + nx + 1, down0, 6)

        def rest0(p):
            return R[p] - ((27.0 + D[p]) * Z[p] - box(Z, p))

        def down1(p):
            s = rest0(2 * p - H) + rest0(2 * p - H + 1)
            return put(R1a, p, mr(ml(LyR, s), RzR))

        loop(H, H + n1x, down1, UR)

        pack1(it, R1a)
        fine1 = [level1(ex, it, 5)]
        start(fine1, FLAT + PACKED)

        Z1[H - 3 : H - 1] = none
        Z1[H + n1x + 1 : H + n1x + 3] = none

        def z1a(p):
            return put(Z1, p, (M1[...] * xin1(p)) * smooth1(R1a, p))

        loop(H - 1, H + n1x + 1, z1a, 5)

        def rest1(p):
            return R1a[p] - ((27.0 + D1[p]) * Z1[p] - box(Z1, p))

        tile[it, 0:n2y] = coarsen(rest1)
        low = coarse_tile(box(Z1, H - 2) + rest1(H - 1))
        high = coarse_tile(rest1(H + n1x) + box(Z1, H + n1x + 1))
        low, high = (jnp.where(lane < 2 * n2z, v, pltpu.roll(v, n2y // 2, 0)) for v in (low, high))
        ring2 = jnp.where(lane // n2z % 2 == 0, low, high)
        tile[it, n2y : n2y + n2y // 2] = ring2[0 : n2y // 2]
        gather_start(1 + it)

        far(it)
        for lo, hi in ((H - 3, H - 1), (H + nx + 1, H + nx + 3)):
            loop(lo, hi, down0, 2)

        finish(fine1, FLAT + PACKED)
        merge1(it, 5, R1)
        if it == 0:
            finish([level1(6, 2, 4)], FLAT + PACKED)
            merge1(2, 4, D1, False)

        def z1b(p):
            return put(Z1, p, (M1[...] * xin1(p)) * smooth1(R1, p))

        loop(H - 4, H + n1x + 4, z1b, U1)

        if it == 0:
            gather_finish(0)
            spread(lambda n, r: eslots[n], E, False)
        gather_finish(1 + it)
        spread(lambda n, r: slots[it, n, n2y:] if r else slots[it, n, 0:n2y], G, True)
        coarse()

        def up1(q):
            v = mr(ml(LyP2, Q[ix * n2x + q]), RzP2)
            p = H - 4 + 2 * q
            a, b = put(Z1, p, Z1[p] + v), put(Z1, p + 1, Z1[p + 1] + v)
            return lambda: (a(), b())

        loop(0, n2x + 4, up1, 4)

        def t1(p):
            return put(T1, p, (M1[...] * xin1(p)) * (R1[p] - ((27.0 + D1[p]) * Z1[p] - box(Z1, p))))

        loop(H - 3, H + n1x + 3, t1, U1)

        def z1c(p):
            return put(Z1, p, Z1[p] + (M1[...] * xin1(p)) * smooth1(T1, p))

        loop(H - 2, H + n1x + 2, z1c, U1)

        def up0(p):
            v = mr(ml(LyP, Z1[p]), RzP)
            q = 2 * p - H
            a, b = put(Z, q, Z[q] + v), put(Z, q + 1, Z[q + 1] + v)
            return lambda: (a(), b())

        loop(H - 2, H + n1x + 2, up0, UR)

        def t0(p):
            return put(T, p, (M0[...] * xin0(p)) * rest0(p))

        loop(H - 2, H + nx + 2, t0, UF)

        def z0(p):
            return put(Z, p, Z[p] + (M0[...] * xin0(p)) * (T[p] * (k3 - k2 * D[p]) + k2 * box(T, p)))

        loop(H - 1, H + nx + 1, z0, UF)

    core = (slice(H, H + ny), slice(0, nz))

    def products(it):
        def one(x, carry):
            p = x + H
            z = Z[p]
            w = ((27.0 + D[p]) * z - box(Z, p))[core[0], core[1]]
            z = z[core[0], core[1]]
            W[it, x] = w
            S0[it, x] = z
            r = R[p, core[0], core[1]]
            out = [carry[0] + r * z, carry[1] + z * w]
            if it:
                out.append(carry[2] + z * W[0, x])
            return tuple(out)

        def body(i, carry):
            for k in range(UP):
                carry = one(i * UP + k, carry)
            return carry

        init = tuple(jnp.zeros((ny, nz), F32) for _ in range(3 if it else 2))
        sums = lax.fori_loop(0, nx // UP, body, init)
        v = jnp.zeros((1, LANES), F32)
        for i, s in enumerate(sums):
            s = jnp.sum(jnp.sum(s, axis=0, keepdims=True), axis=1, keepdims=True)
            v = jnp.where(lane == i, s, v)
        row[it] = v
        gather_start(3 + it)

    def total(k):
        gather_finish(k)

        def body(n, acc):
            return acc + rows[k - 3, n]

        acc = lax.fori_loop(0, N, body, jnp.zeros((1, LANES), F32))
        return acc[:, 0:1], acc[:, 1:2], acc[:, 2:3]

    def far(it):
        if it == 0:
            finish(both, WIDER, 1)
            merge0(0, d_ref, put_d, True)
            merge0(1, x_ref, put_r, True)
        else:
            finish(image, WIDER, 1)
            merge0(2, W.at[0], put_image, True)

    precondition(0)
    products(0)
    image = [fine(2, 2, W.at[0])]
    start(image, FLAT)
    pack0(2, W.at[0])
    start(image, PACKED)
    start(image, WIDER, 1)
    rz0, curve0, _ = total(3)
    alpha0 = rz0 / curve0
    finish(image, FLAT + PACKED)

    def put_image(p, v):
        return put(R, p, R[p] - alpha0 * v)

    merge0(2, W.at[0], put_image)
    precondition(1)
    products(1)
    rz1, zw, zq = total(4)
    beta = rz1 / rz0
    curve = zw + 2.0 * beta * zq + beta * beta * curve0
    alpha = rz1 / curve

    def last(x):
        z = S0[0, x]
        sol_ref[x] = alpha0 * z + alpha * (S0[1, x] + beta * z)
        res_ref[x] = R[x + H, core[0], core[1]] - alpha * (W[1, x] + beta * W[0, x])
        return lambda: None

    loop(0, nx, last, 4)
    drain()
    for k in range(5):
        gather_drain(k)


def solution(mesh):
    dims = (mesh.shape["gx"], mesh.shape["gy"], mesh.shape["gz"])
    N = dims[0] * dims[1] * dims[2]

    def local(right_side, diagonal):
        nx, ny, nz = right_side.shape
        assert nz == LANES and nx * H == LANES and (nx // 4) * (nz // 4) == LANES and ny == 32
        n1x, n1y, n2y = nx // 2, ny // 2, ny // 4
        X0, Y0, X1, Y1 = nx + 2 * H, ny + 2 * H, n1x + 2 * H, n1y + 2 * H
        NX2, NY2, NZ2 = dims[0] * nx // 4, dims[1] * n2y, dims[2] * nz // 4
        W0 = 2 * LANES
        vm = lambda *s: pltpu.VMEM(s, F32)
        vb = lambda *s: pltpu.VMEM(s, BF16)
        dma = pltpu.SemaphoreType.DMA
        scratch = [
            vm(nx, ny, nz), vm(nx, ny, nz),
            vm(3, X0, Y0, LANES), vm(3, 2, 3, Y0, LANES), vm(3, 2, ny, LANES),
            vm(3, 2, 2, H, LANES), vm(3, 2, 2, 3, H, LANES),
            vm(X0, Y0, W0), vm(X0, Y0, W0), vm(X0, Y0, W0), vm(X0, Y0, W0),
            vm(2, nx, ny, nz), vm(2, nx, ny, nz),
            vm(3, X1, Y1, LANES), vm(3, 2, 3, Y1, LANES), vm(3, n1y, LANES),
            vm(X1, Y1, LANES), vm(X1, Y1, LANES), vm(X1, Y1, LANES), vm(X1, Y1, LANES), vm(X1, Y1, LANES),
            vm(3, n1x, n1y, LANES),
            vm(2, N, n2y * 3 // 2, LANES), vm(2, n2y * 3 // 2, LANES), vm(N, n2y, LANES), vm(n2y, LANES), vm(2, N, 1, LANES), vm(2, 1, LANES),
            vm(NX2 + 4, NY2, NZ2), vm(NX2 + 4, NY2, NZ2), vm(NX2 + 4, NY2, NZ2), vm(NX2 + 4, NY2, NZ2),
            vm(Y0, W0), vm(Y1, LANES),
            vb(Y1, 2 * Y0), vb(W0, LANES), vb(Y0, 2 * Y1), vb(LANES, W0),
            vb(n2y, 2 * Y1), vb(LANES, LANES), vb(Y1, 2 * NY2), vb(NZ2, LANES),
            vm(256, H, LANES), dma((7,)), dma((7,)), dma((5,)), dma((5,)), dma((2,)),
        ]
        shape = jax.ShapeDtypeStruct(right_side.shape, F32)
        return pl.pallas_call(
            functools.partial(kernel, dims),
            out_shape=(shape, shape),
            in_specs=[pl.BlockSpec(memory_space=pl.ANY)] * 2,
            out_specs=[pl.BlockSpec(memory_space=pltpu.VMEM)] * 2,
            scratch_shapes=scratch,
            compiler_params=pltpu.CompilerParams(collective_id=0, has_side_effects=True),
        )(right_side, diagonal)

    placed = (P("gx", "gy", "gz"), P("gx", "gy", "gz"))
    return jax.shard_map(local, mesh=mesh, in_specs=placed, out_specs=placed, check_vma=False)
```

```python
import functools
import math

import jax
import jax.numpy as jnp
from jax import lax
from jax.experimental import pallas as pl
from jax.experimental.pallas import tpu as pltpu
from jax.sharding import PartitionSpec as P

ITERS = 2
LANES = 128
H = 8
MESH = pl.DeviceIdType.MESH
F32 = jnp.float32
UF, UR, U1, UC, UM, UP = 4, 4, 4, 8, 4, 4
OFFSETS = [
    (a, b, c) for a in (-1, 0, 1) for b in (-1, 0, 1) for c in (-1, 0, 1) if (a, b, c) != (0, 0, 0)
]
OFFSETS.sort(key=lambda o: (o[0] == 0, o[2] == 0, o[1] == 0))


def cheb_terms(lower):
    upper = 58.0
    theta = (upper + lower) / 2.0
    delta = (upper - lower) / 2.0
    return theta, delta, theta / delta


def cheb_two(lower):
    theta, delta, sigma = cheb_terms(lower)
    rho = 1.0 / sigma
    rho_next = 1.0 / (2.0 * sigma - rho)
    gain = 2.0 * rho_next / delta
    k2 = gain / theta
    k3 = (1.0 + rho_next * rho) / theta + gain - 27.0 * k2
    return k2, k3


def take(v, index):
    return jnp.take_along_axis(v, jnp.broadcast_to(index, v.shape), axis=1, mode="promise_in_bounds")


def iota(shape, dim):
    return lax.broadcasted_iota(jnp.int32, shape, dim)


def ring(s, rows, lanes):
    s = s + pltpu.roll(s, 1, 0) + pltpu.roll(s, rows - 1, 0)
    return s + pltpu.roll(s, 1, 1) + pltpu.roll(s, lanes - 1, 1)


def box(ref, p):
    s = ref[p - 1] + ref[p] + ref[p + 1]
    return ring(s, *s.shape)


def kernel(
    dims, x_hbm, d_hbm, sol_ref, res_ref,
    x_ref, d_ref, land, edge, face, corner, cland, D, R, Z, T, W, S0,
    land1, edge1, face1, D1, R1a, R1, Z1, T1, send1,
    slots, tile, eslots, etile, rows, row, G, E, Y, Q, QP, S, M0, M1,
    spare, ssem, rsem, gssem, grsem, csem,
):
    GX, GY, GZ = dims
    N = GX * GY * GZ
    nx, ny, nz = x_ref.shape
    n1x, n1y, n1z = nx // 2, ny // 2, nz // 2
    n2x, n2y, n2z = nx // 4, ny // 4, nz // 4
    Y0, Y1 = ny + 2 * H, n1y + 2 * H
    NX2, NY2, NZ2 = GX * n2x, GY * n2y, GZ * n2z
    ix, iy, iz = lax.axis_index("gx"), lax.axis_index("gy"), lax.axis_index("gz")
    me = (ix * GY + iy) * GZ + iz
    k2, k3 = cheb_two(7.0)
    W0 = 2 * LANES

    FAR = (3, 4, 4)
    NEAR = 2
    DEEP = LANES // ny

    def device(n):
        return {"gx": n // (GY * GZ), "gy": (n // GZ) % GY, "gz": n % GZ}

    loads = [
        pltpu.make_async_copy(src, dst, csem.at[i])
        for i, (src, dst) in enumerate(((d_hbm, d_ref), (x_hbm, x_ref)))
    ]
    barrier = pltpu.get_barrier_semaphore()

    def greet(d, _):
        pl.semaphore_signal(barrier, inc=1, device_id=device((me + d) % N), device_id_type=MESH)
        return 0

    lax.fori_loop(1, N, greet, 0)
    for load in loads:
        load.start()

    def cut(o, n, h):
        if o == 0:
            return 0, H, n
        if o > 0:
            return n - h, H - h, h
        return 0, H + n, h

    def there(o, sign):
        ok = None
        for i, g, d in ((ix, GX, o[0]), (iy, GY, o[1]), (iz, GZ, o[2])):
            d = d * sign
            if d:
                t = (i + d >= 0) & (i + d < g)
                ok = t if ok is None else ok & t
        return ok

    def remote(ex, o, src, dst):
        return pltpu.make_async_remote_copy(
            src_ref=src, dst_ref=dst, send_sem=ssem.at[ex], recv_sem=rsem.at[ex],
            device_id={"gx": ix + o[0], "gy": iy + o[1], "gz": iz + o[2]}, device_id_type=MESH,
        )

    def fine(ex, e, core):
        def make(k, far):
            o = a, b, c = OFFSETS[k]
            ys, yd, yn = cut(b, ny, H)
            if c == 0:
                if a == 0:
                    xs, xd, xn = 0, H, nx
                else:
                    lo, hi = (NEAR, FAR[e]) if far else (0, NEAR)
                    xs, xd, xn = (nx - hi, H - hi, hi - lo) if a > 0 else (lo, H + nx + lo, hi - lo)
                src = core.at[pl.ds(xs, xn), pl.ds(ys, yn)]
                dst = land.at[e, pl.ds(xd, xn), pl.ds(yd, yn)]
            else:
                f, side = (1, 0) if c > 0 else (0, 1)
                if a == 0:
                    src, dst = face.at[e, f, pl.ds(ys, yn)], edge.at[e, side, 1, pl.ds(yd, yn)]
                else:
                    src, dst = corner.at[e, (1 - a) // 2, f], cland.at[e, side, (1 - a) // 2, 1 - b]
            return ex + far, o, src, dst
        return make

    def level1(ex, e, h):
        def make(k, far):
            o = a, b, c = OFFSETS[k]
            xs, xd, xn = cut(a, n1x, h)
            ys, yd, yn = cut(b, n1y, H)
            if c == 0:
                src = send1.at[e, pl.ds(xs, xn), pl.ds(ys, yn)]
                dst = land1.at[e, pl.ds(xd, xn), pl.ds(yd, yn)]
            else:
                src, dst = face1.at[e, pl.ds(ys, yn)], edge1.at[e, 0 if c > 0 else 1, 1 - a, pl.ds(yd, yn)]
            return ex, o, src, dst
        return make

    FLAT = [k for k, o in enumerate(OFFSETS) if o[2] == 0]
    PACKED = [k for k, o in enumerate(OFFSETS) if o[2] != 0]
    WIDER = [k for k, o in enumerate(OFFSETS) if o[2] == 0 and o[0] != 0]
    sent = []

    def start(makers, ks, far=0):
        for k in ks:
            @pl.when(there(OFFSETS[k], 1))
            def _():
                for make in makers:
                    remote(*make(k, far)).start()

    def counts(i, g):
        if g < 3:
            return [(g - 1, None)]
        outer = (i == 0) | (i == g - 1)
        return [(1, outer), (2, jnp.logical_not(outer))]

    def settle(makers, ks, far, received):
        for cx, px in counts(ix, GX):
            for cy, py in counts(iy, GY):
                for cz, pz in counts(iz, GZ):
                    n = 0
                    for k in ks:
                        a, b, c = OFFSETS[k]
                        if min(a, b, c) >= 0:
                            times = (cx if a else 1) * (cy if b else 1) * (cz if c else 1)
                            for make in makers:
                                n += times * math.prod(make(k, far)[2].shape) // (H * LANES)
                    if n == 0:
                        continue
                    some = spare.at[pl.ds(0, n)]
                    copy = remote(makers[0](0, far)[0], (0, 0, 1), some, some)
                    wait = copy.wait_recv if received else copy.wait_send
                    ok = [p for p in (px, py, pz) if p is not None]
                    if ok:
                        pl.when(functools.reduce(jnp.logical_and, ok))(wait)
                    else:
                        wait()

    def finish(makers, ks, far=0):
        settle(makers, ks, far, True)
        sent.append((makers, ks, far))

    def drain():
        for makers, ks, far in sent:
            settle(makers, ks, far, False)

    def ends(k, sender):
        if k == 0:
            return etile, eslots.at[sender]
        if k < 3:
            return tile.at[k - 1], slots.at[k - 1, sender]
        return row.at[k - 3], rows.at[k - 3, sender]

    def gather_start(k):
        src, dst = ends(k, me)

        def body(d, _):
            pltpu.make_async_remote_copy(
                src_ref=src, dst_ref=dst, send_sem=gssem.at[k], recv_sem=grsem.at[k],
                device_id=device((me + d) % N), device_id_type=MESH,
            ).start()
            return 0
        lax.fori_loop(1, N, body, 0)
        dst[...] = src[...]

    def everyone(k):
        some = pl.ds(0, N - 1)
        ref = eslots.at[some] if k == 0 else slots.at[k - 1, some] if k < 3 else rows.at[k - 3, some]
        return pltpu.make_async_remote_copy(
            src_ref=ref, dst_ref=ref, send_sem=gssem.at[k], recv_sem=grsem.at[k],
            device_id=device((me + 1) % N), device_id_type=MESH,
        )

    def gather_finish(k):
        everyone(k).wait_recv()

    def gather_drain(k):
        everyone(k).wait_send()

    lane = iota((1, LANES), 1)

    def pack0(e, core):
        first = jnp.zeros((ny, LANES), F32)
        last = jnp.zeros((ny, LANES), F32)
        for x in range(nx):
            v = core[x]
            here = (lane >= H * x) & (lane < H * x + H)
            first = jnp.where(here, pltpu.roll(v, H * x, 1) if x else v, first)
            last = jnp.where(here, pltpu.roll(v, (H * x + H) % LANES, 1) if (H * x + H) % LANES else v, last)
        for f, v in enumerate((first, last)):
            face[e, f] = v
            for i, base in enumerate((nx - DEEP, 0)):
                fold = jnp.zeros((H, LANES), F32)
                for k in range(ny // H):
                    lo = H * DEEP * k
                    shift = (lo - H * base) % LANES
                    part = v[H * k : H * k + H]
                    part = pltpu.roll(part, shift, 1) if shift else part
                    fold = jnp.where((lane >= lo) & (lane < lo + H * DEEP), part, fold)
                corner[e, i, f] = fold

    def unfold(e):
        for side in range(2):
            for i in range(2):
                for k in range(-1, ny // H + 1):
                    v = cland[e, side, i, 0 if k < 0 else 2 if k == ny // H else 1]
                    shift = -H * DEEP * (k % (ny // H)) % LANES
                    edge[e, side, 2 * i, H * k + H : H * k + 2 * H] = pltpu.roll(v, shift, 1) if shift else v

    pl.semaphore_wait(barrier, N - 1)
    for load in loads:
        load.wait()
    both = [fine(0, 0, d_ref), fine(0, 1, x_ref)]
    start(both, FLAT)
    pack0(0, d_ref)
    pack0(1, x_ref)
    start(both, PACKED)
    start(both, WIDER, 1)

    def off0(l):
        return jnp.where(l < 192, l, l - 256)

    def off1(l):
        return jnp.where(l < 96, l, l - 128)

    def inside(v, i, n, g):
        v = v + i * n
        return (v >= 0) & (v < g * n)

    def f(cond, value=1.0):
        return jnp.where(cond, F32(value), F32(0.0))

    def near0(z):
        return (z >= -H) & (z < nz + H)

    def near1(z):
        return (z >= -H) & (z < n1z + H)

    yy, zz = iota((Y0, W0), 0) - H, off0(iota((Y0, W0), 1))
    M0[...] = f(inside(yy, iy, ny, GY) & inside(zz, iz, nz, GZ) & near0(zz))
    yy, zz = iota((Y1, LANES), 0) - H, off1(iota((Y1, LANES), 1))
    M1[...] = f(inside(yy, iy, n1y, GY) & inside(zz, iz, n1z, GZ) & near1(zz))
    everywhere = iota((1, LANES), 1)
    evens, halved = everywhere * 2 % LANES, everywhere // 2
    blocks = everywhere % n2z * 2
    MID = slice(H // 2, H // 2 + Y0 // 2)

    def put_halves(p, v):
        def store():
            S[0, p] = v[:, :LANES]
            S[1, p] = v[:, LANES:]
        return store

    def shrink0(p):
        def half(h):
            v = S[h, p, pl.ds(0, Y0 // 2, stride=2)] + S[h, p, pl.ds(1, Y0 // 2, stride=2)]
            return take(v + pltpu.roll(v, LANES - 1, 1), evens)
        return jnp.where(everywhere < n1z, half(0), half(1))

    def put_mid(ref, p, v):
        def store():
            ref[p, MID] = v
        return store

    def shrink1(src, p):
        v = src[p, pl.ds(H, n2y, stride=2)] + src[p, pl.ds(H + 1, n2y, stride=2)]
        return 0.5 * take(v + pltpu.roll(v, LANES - 1, 1), blocks)

    def xin0(p):
        return f(inside(p - H, ix, nx, GX))

    def xin1(p):
        return f(inside(p - H, ix, n1x, GX))

    def loop(lo, hi, body, group=1):
        count = hi - lo
        while count % group:
            group -= 1

        def step(i, _):
            stores = [body(lo + i * group + k) for k in range(group)]
            for store in stores:
                store()
            return 0
        if count == group:
            step(0, 0)
        else:
            lax.fori_loop(0, count // group, step, 0)

    def put(ref, p, v):
        def store():
            ref[p] = v
        return store

    def merged0(e, core, p, b, sx):
        right = pltpu.roll(edge[e, 1, b], (LANES - H * sx) % LANES, 1)
        left = pltpu.roll(edge[e, 0, b], (2 * LANES - H - H * sx) % LANES, 1)
        return land[e, p], jnp.where(lane < H, right, left)

    def merge0(e, core, emit, far=False):
        near = ((0, H - NEAR, H, DEEP - H), (1, H, H + nx, -H), (2, H + nx, H + nx + NEAR, -H - nx))
        rest = ((0, H - FAR[e], H - NEAR, DEEP - H), (2, H + nx + NEAR, H + nx + FAR[e], -H - nx))
        if not far:
            unfold(e)
            land[e, H : H + nx, H : H + ny] = core[...]
        for b, lo, hi, shift in rest if far else near:
            def body(p, b=b, shift=shift):
                t0, t1 = merged0(e, core, p, b, p + shift)
                ok = M0[...] * xin0(p) > 0.5
                return emit(p, jnp.where(ok, jnp.concatenate([t0, t1], axis=1), 0.0))
            loop(lo, hi, body, UM)

    none = jnp.zeros((2, Y1, LANES), F32)
    R1a[...] = jnp.zeros(R1a.shape, F32)
    D1[...] = jnp.zeros(D1.shape, F32)
    QP[...] = jnp.zeros(QP.shape, F32)

    def put_d(p, v):
        return put(D, p, v)

    def put_r(p, v):
        return put(R, p, v)

    finish(both, FLAT + PACKED)
    merge0(0, d_ref, put_d)
    merge0(1, x_ref, put_r)

    def pair_d(p):
        return put_halves(p, D[2 * p - H] + D[2 * p - H + 1])

    def make_d1(p):
        return put_mid(D1, p, 0.125 * shrink0(p))

    loop(H - 1, H + n1x + 1, pair_d, 5)
    loop(H - 1, H + n1x + 1, make_d1, 5)

    def pack1(e, src):
        edges = jnp.zeros((n1y, LANES), F32)
        for x in range(n1x):
            v = src[H + x, H : H + n1y]
            send1[e, x] = v
            lo = 2 * H * x
            low = pltpu.roll(v, lo, 1) if lo else v
            up = pltpu.roll(v, (lo + 2 * H - n1z) % LANES, 1) if (lo + 2 * H - n1z) % LANES else v
            edges = jnp.where((lane >= lo) & (lane < lo + H), low, edges)
            edges = jnp.where((lane >= lo + H) & (lane < lo + 2 * H), up, edges)
        face1[e] = edges

    def merge1(e, h, dst, inner=True):
        land1[e, H : H + n1x, H : H + n1y] = send1[e]
        for b, lo, hi, shift in (
            (0, H - h, H, n1x - H), (1, H, H + n1x, -H), (2, H + n1x, H + n1x + h, -H - n1x)
        ):
            if b == 1 and not inner:
                continue

            def body(p, b=b, shift=shift):
                sx = p + shift
                right = pltpu.roll(edge1[e, 1, b], (LANES + n1z - 2 * H * sx) % LANES, 1)
                left = pltpu.roll(edge1[e, 0, b], (2 * LANES - 2 * H - 2 * H * sx) % LANES, 1)
                v = jnp.where(lane < n1z, land1[e, p], jnp.where(lane < n1z + H, right, left))
                return put(dst, p, jnp.where(M1[...] * xin1(p) > 0.5, v, 0.0))
            loop(lo, hi, body, 5)

    pack1(2, D1)
    start([level1(6, 2, 4)], FLAT + PACKED)

    def coarsen(plane):
        total = jnp.zeros((n2y, LANES), F32)
        for x in range(n2x):
            T1[x] = plane(H + 2 * x) + plane(H + 2 * x + 1)
        for x in range(n2x):
            total = total + jnp.where((lane >= n2z * x) & (lane < n2z * x + n2z), shrink1(T1, x), 0.0)
        return total

    etile[...] = coarsen(lambda p: D1[p]) * 0.25
    gather_start(0)

    def block(src, q, at):
        shift = (n2z * (q - at)) % LANES
        return pltpu.roll(src, shift, 1) if shift else src

    def along(load, at):
        v = None
        for q in range(LANES // n2z):
            part = block(load(q), q, at)
            v = part if v is None else jnp.where(lane >= n2z * q, part, v)
        return v

    PER = LANES // n2z

    def spread(load, dst, ring):
        def body(a):
            for x in range(n2x):
                for b in range(GY):
                    for t in range(NZ2 // LANES):
                        v = along(lambda q: load((a * GY + b) * GZ + t * PER + q, 0), x)
                        dst[a * n2x + x + 2, n2y * b : n2y * b + n2y, LANES * t : LANES * t + LANES] = v
            return lambda: None
        loop(0, GX, body)
        if not ring:
            return

        def edges(a):
            for b in range(GY):
                for t in range(NZ2 // LANES):
                    for i, p in ((0, a * n2x + 1), (1, (a + 1) * n2x + 2)):
                        v = jnp.concatenate([
                            along(lambda q: load((a * GY + b) * GZ + t * PER + q, 1), i + h) for h in (0, 2)
                        ], axis=0)
                        at = (p, slice(n2y * b, n2y * b + n2y), slice(LANES * t, LANES * t + LANES))
                        dst[at] = dst[at] + v
            return lambda: None
        loop(0, GX, edges)
        zero = jnp.zeros((NY2, NZ2), F32)
        dst[1] = zero
        dst[NX2 + 2] = zero

    rows2, lanes2 = iota((NY2, NZ2), 0), iota((NY2, NZ2), 1)

    def box2(ref, p):
        s = ref[p - 1] + ref[p] + ref[p + 1]
        s = (
            s
            + jnp.where(rows2 > 0, pltpu.roll(s, 1, 0), 0.0)
            + jnp.where(rows2 < NY2 - 1, pltpu.roll(s, NY2 - 1, 0), 0.0)
        )
        return (
            s
            + jnp.where(lanes2 > 0, pltpu.roll(s, 1, 1), 0.0)
            + jnp.where(lanes2 < NZ2 - 1, pltpu.roll(s, NZ2 - 1, 1), 0.0)
        )

    zero2 = jnp.zeros((2, NY2, NZ2), F32)
    for ref in (G, Q, Y):
        ref[0:2] = zero2
        ref[NX2 + 2 : NX2 + 4] = zero2

    def coarse():
        theta, delta, sigma = cheb_terms(1.0)
        rho1 = 1.0 / sigma
        rho2 = 1.0 / (2.0 * sigma - rho1)
        rho3 = 1.0 / (2.0 * sigma - rho2)
        a2, b2 = rho2 * rho1, 2.0 * rho2 / delta
        a3, b3 = rho3 * rho2, 2.0 * rho3 / delta

        def first(p):
            g = G[p]
            remain = g - ((27.0 + E[p]) * g - box2(G, p)) * (1.0 / theta)
            a, b = put(Q, p, (a2 / theta) * g + b2 * remain), put(Y, p, remain)
            return lambda: (a(), b())

        def second(p):
            q, g = Q[p], G[p]
            remain = Y[p] - ((27.0 + E[p]) * q - box2(Q, p))
            return put(Y, p, (1.0 / theta) * g + (1.0 + a3) * q + b3 * remain)

        def third(p):
            y = Y[p]
            left = G[p] - ((27.0 + E[p]) * y - box2(Y, p))
            shift = jnp.sum(left, axis=1, keepdims=True) / jnp.sum(1.0 + E[p], axis=1, keepdims=True)
            def store():
                QP[p, H : H + NY2] = y + shift
            return store

        for body in (first, second, third):
            loop(2, NX2 + 2, body, UC)

    def smooth1(ref, p):
        return ref[p] * (k3 - k2 * D1[p]) + k2 * box(ref, p)

    def precondition(it):
        ex = 4 + it

        def down0(p):
            return put(Z, p, (M0[...] * xin0(p)) * (R[p] * (k3 - k2 * D[p]) + k2 * box(R, p)))

        loop(H - 1, H + nx + 1, down0, 6)

        def rest0(p):
            return R[p] - ((27.0 + D[p]) * Z[p] - box(Z, p))

        def pair0(p):
            return put_halves(p, rest0(2 * p - H) + rest0(2 * p - H + 1))

        def down1(p):
            return put_mid(R1a, p, 0.5 * M1[MID] * shrink0(p))

        loop(H, H + n1x, pair0, 2)
        loop(H, H + n1x, down1, 8)

        pack1(it, R1a)
        fine1 = [level1(ex, it, 5)]
        start(fine1, FLAT + PACKED)

        Z1[H - 3 : H - 1] = none
        Z1[H + n1x + 1 : H + n1x + 3] = none

        def z1a(p):
            return put(Z1, p, (M1[...] * xin1(p)) * smooth1(R1a, p))

        loop(H - 1, H + n1x + 1, z1a, 5)

        def rest1(p):
            return R1a[p] - ((27.0 + D1[p]) * Z1[p] - box(Z1, p))

        tile[it, 0:n2y] = coarsen(rest1)
        T1[n2x] = box(Z1, H - 2) + rest1(H - 1)
        T1[n2x + 1] = rest1(H + n1x) + box(Z1, H + n1x + 1)
        low, high = shrink1(T1, n2x), shrink1(T1, n2x + 1)
        low, high = (jnp.where(lane < 2 * n2z, v, pltpu.roll(v, n2y // 2, 0)) for v in (low, high))
        ring2 = jnp.where(lane // n2z % 2 == 0, low, high)
        tile[it, n2y : n2y + n2y // 2] = ring2[0 : n2y // 2]
        gather_start(1 + it)

        far(it)
        for lo, hi in ((H - 3, H - 1), (H + nx + 1, H + nx + 3)):
            loop(lo, hi, down0, 2)

        finish(fine1, FLAT + PACKED)
        merge1(it, 5, R1)
        if it == 0:
            finish([level1(6, 2, 4)], FLAT + PACKED)
            merge1(2, 4, D1, False)

        def z1b(p):
            return put(Z1, p, (M1[...] * xin1(p)) * smooth1(R1, p))

        loop(H - 4, H + n1x + 4, z1b, U1)

        if it == 0:
            gather_finish(0)
            spread(lambda n, r: eslots[n], E, False)
        gather_finish(1 + it)
        spread(lambda n, r: slots[it, n, n2y:] if r else slots[it, n, 0:n2y], G, True)
        coarse()

        zz = off1(everywhere)
        source = (zz + iz * n1z) // 2
        fits = inside(zz, iz, n1z, GZ) & near1(zz)

        def wide1(q):
            rows2 = pl.ds(pl.multiple_of(iy * n2y, H), n2y + 2 * H)
            v = jnp.zeros((n1y, LANES), F32)
            for t in range(NZ2 // LANES):
                part = QP[ix * n2x + q, rows2, LANES * t : LANES * t + LANES][H // 2 : H // 2 + n1y]
                at = source - LANES * t
                v = jnp.where(fits & (at >= 0) & (at < LANES), take(part, jnp.clip(at, 0, LANES - 1)), v)

            def store():
                T1[q, pl.ds(0, n1y, stride=2)] = v
                T1[q, pl.ds(1, n1y, stride=2)] = v
            return store

        def up1(q):
            v = T1[q]
            p = H - 4 + 2 * q
            a, b = put(Z1, p, Z1[p] + v), put(Z1, p + 1, Z1[p + 1] + v)
            return lambda: (a(), b())

        loop(0, n2x + 4, wide1, 8)
        loop(0, n2x + 4, up1, 4)

        def t1(p):
            return put(T1, p, (M1[...] * xin1(p)) * (R1[p] - ((27.0 + D1[p]) * Z1[p] - box(Z1, p))))

        loop(H - 3, H + n1x + 3, t1, U1)

        def z1c(p):
            return put(Z1, p, Z1[p] + (M1[...] * xin1(p)) * smooth1(T1, p))

        loop(H - 2, H + n1x + 2, z1c, U1)

        def wide0(p):
            v = Z1[p, MID]
            parts = take(v, halved), take(v, halved + n1z)

            def store():
                for h, part in enumerate(parts):
                    S[h, p, pl.ds(0, Y0 // 2, stride=2)] = part
                    S[h, p, pl.ds(1, Y0 // 2, stride=2)] = part
            return store

        def up0(p):
            v = jnp.concatenate([S[0, p], S[1, p]], axis=1)
            q = 2 * p - H
            a, b = put(Z, q, Z[q] + v), put(Z, q + 1, Z[q + 1] + v)
            return lambda: (a(), b())

        loop(H - 2, H + n1x + 2, wide0, 4)
        loop(H - 2, H + n1x + 2, up0, 4)

        def t0(p):
            return put(T, p, (M0[...] * xin0(p)) * rest0(p))

        loop(H - 2, H + nx + 2, t0, UF)

        def z0(p):
            return put(Z, p, Z[p] + (M0[...] * xin0(p)) * (T[p] * (k3 - k2 * D[p]) + k2 * box(T, p)))

        loop(H - 1, H + nx + 1, z0, UF)

    core = (slice(H, H + ny), slice(0, nz))

    def products(it):
        def one(x, carry):
            p = x + H
            z = Z[p]
            w = ((27.0 + D[p]) * z - box(Z, p))[core[0], core[1]]
            z = z[core[0], core[1]]
            W[it, x] = w
            S0[it, x] = z
            r = R[p, core[0], core[1]]
            out = [carry[0] + r * z, carry[1] + z * w]
            if it:
                out.append(carry[2] + z * W[0, x])
            return tuple(out)

        def body(i, carry):
            for k in range(UP):
                carry = one(i * UP + k, carry)
            return carry

        init = tuple(jnp.zeros((ny, nz), F32) for _ in range(3 if it else 2))
        sums = lax.fori_loop(0, nx // UP, body, init)
        v = jnp.zeros((1, LANES), F32)
        for i, s in enumerate(sums):
            s = jnp.sum(jnp.sum(s, axis=0, keepdims=True), axis=1, keepdims=True)
            v = jnp.where(lane == i, s, v)
        row[it] = v
        gather_start(3 + it)

    def total(k):
        gather_finish(k)

        def body(n, acc):
            return acc + rows[k - 3, n]

        acc = lax.fori_loop(0, N, body, jnp.zeros((1, LANES), F32))
        return acc[:, 0:1], acc[:, 1:2], acc[:, 2:3]

    def far(it):
        if it == 0:
            finish(both, WIDER, 1)
            merge0(0, d_ref, put_d, True)
            merge0(1, x_ref, put_r, True)
        else:
            finish(image, WIDER, 1)
            merge0(2, W.at[0], put_image, True)

    precondition(0)
    products(0)
    image = [fine(2, 2, W.at[0])]
    start(image, FLAT)
    pack0(2, W.at[0])
    start(image, PACKED)
    start(image, WIDER, 1)
    rz0, curve0, _ = total(3)
    alpha0 = rz0 / curve0
    finish(image, FLAT + PACKED)

    def put_image(p, v):
        return put(R, p, R[p] - alpha0 * v)

    merge0(2, W.at[0], put_image)
    precondition(1)
    products(1)
    rz1, zw, zq = total(4)
    beta = rz1 / rz0
    curve = zw + 2.0 * beta * zq + beta * beta * curve0
    alpha = rz1 / curve

    def last(x):
        z = S0[0, x]
        sol_ref[x] = alpha0 * z + alpha * (S0[1, x] + beta * z)
        res_ref[x] = R[x + H, core[0], core[1]] - alpha * (W[1, x] + beta * W[0, x])
        return lambda: None

    loop(0, nx, last, 4)
    drain()
    for k in range(5):
        gather_drain(k)


def solution(mesh):
    dims = (mesh.shape["gx"], mesh.shape["gy"], mesh.shape["gz"])
    N = dims[0] * dims[1] * dims[2]

    def local(right_side, diagonal):
        nx, ny, nz = right_side.shape
        assert nz == LANES and nx * H == LANES and (nx // 4) * (nz // 4) == LANES and ny == 32
        n1x, n1y, n2y = nx // 2, ny // 2, ny // 4
        X0, Y0, X1, Y1 = nx + 2 * H, ny + 2 * H, n1x + 2 * H, n1y + 2 * H
        NX2, NY2, NZ2 = dims[0] * nx // 4, dims[1] * n2y, dims[2] * nz // 4
        W0 = 2 * LANES
        vm = lambda *s: pltpu.VMEM(s, F32)
        dma = pltpu.SemaphoreType.DMA
        scratch = [
            vm(nx, ny, nz), vm(nx, ny, nz),
            vm(3, X0, Y0, LANES), vm(3, 2, 3, Y0, LANES), vm(3, 2, ny, LANES),
            vm(3, 2, 2, H, LANES), vm(3, 2, 2, 3, H, LANES),
            vm(X0, Y0, W0), vm(X0, Y0, W0), vm(X0, Y0, W0), vm(X0, Y0, W0),
            vm(2, nx, ny, nz), vm(2, nx, ny, nz),
            vm(3, X1, Y1, LANES), vm(3, 2, 3, Y1, LANES), vm(3, n1y, LANES),
            vm(X1, Y1, LANES), vm(X1, Y1, LANES), vm(X1, Y1, LANES), vm(X1, Y1, LANES), vm(X1, Y1, LANES),
            vm(3, n1x, n1y, LANES),
            vm(2, N, n2y * 3 // 2, LANES), vm(2, n2y * 3 // 2, LANES), vm(N, n2y, LANES), vm(n2y, LANES), vm(2, N, 1, LANES), vm(2, 1, LANES),
            vm(NX2 + 4, NY2, NZ2), vm(NX2 + 4, NY2, NZ2), vm(NX2 + 4, NY2, NZ2), vm(NX2 + 4, NY2, NZ2),
            vm(NX2 + 4, NY2 + 2 * H, NZ2), vm(2, X0, Y0, LANES), vm(Y0, W0), vm(Y1, LANES),
            vm(256, H, LANES), dma((7,)), dma((7,)), dma((5,)), dma((5,)), dma((2,)),
        ]
        shape = jax.ShapeDtypeStruct(right_side.shape, F32)
        return pl.pallas_call(
            functools.partial(kernel, dims),
            out_shape=(shape, shape),
            in_specs=[pl.BlockSpec(memory_space=pl.ANY)] * 2,
            out_specs=[pl.BlockSpec(memory_space=pltpu.VMEM)] * 2,
            scratch_shapes=scratch,
            compiler_params=pltpu.CompilerParams(collective_id=0, has_side_effects=True),
        )(right_side, diagonal)

    placed = (P("gx", "gy", "gz"), P("gx", "gy", "gz"))
    return jax.shard_map(local, mesh=mesh, in_specs=placed, out_specs=placed, check_vma=False)
```

```python
import functools
import math

import jax
import jax.numpy as jnp
from jax import lax
from jax.experimental import pallas as pl
from jax.experimental.pallas import tpu as pltpu
from jax.sharding import PartitionSpec as P

ITERS = 2
LANES = 128
H = 8
MESH = pl.DeviceIdType.MESH
F32 = jnp.float32
UF, UR, U1, UC, UM, UP = 4, 4, 4, 6, 4, 4
OFFSETS = [
    (a, b, c) for a in (-1, 0, 1) for b in (-1, 0, 1) for c in (-1, 0, 1) if (a, b, c) != (0, 0, 0)
]
OFFSETS.sort(key=lambda o: (o[0] == 0, o[2] == 0, o[1] == 0))


def cheb_terms(lower):
    upper = 58.0
    theta = (upper + lower) / 2.0
    delta = (upper - lower) / 2.0
    return theta, delta, theta / delta


def cheb_two(lower):
    theta, delta, sigma = cheb_terms(lower)
    rho = 1.0 / sigma
    rho_next = 1.0 / (2.0 * sigma - rho)
    gain = 2.0 * rho_next / delta
    k2 = gain / theta
    k3 = (1.0 + rho_next * rho) / theta + gain - 27.0 * k2
    return k2, k3


def take(v, index):
    return jnp.take_along_axis(v, jnp.broadcast_to(index, v.shape), axis=1, mode="promise_in_bounds")


def iota(shape, dim):
    return lax.broadcasted_iota(jnp.int32, shape, dim)


def ring(s, rows, lanes):
    s = s + pltpu.roll(s, 1, 0) + pltpu.roll(s, rows - 1, 0)
    return s + pltpu.roll(s, 1, 1) + pltpu.roll(s, lanes - 1, 1)


def box(ref, p):
    s = ref[p - 1] + ref[p] + ref[p + 1]
    return ring(s, *s.shape)


def kernel(
    dims, x_hbm, d_hbm, sol_ref, res_ref,
    x_ref, d_ref, land, edge, face, corner, cland, D, R, Z, T, W, S0,
    land1, edge1, face1, D1, R1a, R1, Z1, T1, send1,
    slots, tile, eslots, etile, rows, row, G, E, Y, Q, QP, lines, S, M0, M1,
    spare, ssem, rsem, gssem, grsem, csem,
):
    GX, GY, GZ = dims
    N = GX * GY * GZ
    nx, ny, nz = x_ref.shape
    n1x, n1y, n1z = nx // 2, ny // 2, nz // 2
    n2x, n2y, n2z = nx // 4, ny // 4, nz // 4
    Y0, Y1 = ny + 2 * H, n1y + 2 * H
    NX2, NY2, NZ2 = GX * n2x, GY * n2y, GZ * n2z
    ix, iy, iz = lax.axis_index("gx"), lax.axis_index("gy"), lax.axis_index("gz")
    me = (ix * GY + iy) * GZ + iz
    k2, k3 = cheb_two(7.0)
    W0 = 2 * LANES

    FAR = (3, 4, 4)
    NEAR = 2
    DEEP = LANES // ny

    def device(n):
        n = lax.rem(n, N)
        return {"gx": lax.div(n, GY * GZ), "gy": lax.rem(lax.div(n, GZ), GY), "gz": lax.rem(n, GZ)}

    loads = [
        pltpu.make_async_copy(src, dst, csem.at[i])
        for i, (src, dst) in enumerate(((d_hbm, d_ref), (x_hbm, x_ref)))
    ]
    barrier = pltpu.get_barrier_semaphore()

    def greet(d, _):
        pl.semaphore_signal(barrier, inc=1, device_id=device(me + d), device_id_type=MESH)
        return 0

    lax.fori_loop(1, N, greet, 0)
    for load in loads:
        load.start()

    def cut(o, n, h):
        if o == 0:
            return 0, H, n
        if o > 0:
            return n - h, H - h, h
        return 0, H + n, h

    def there(o, sign):
        ok = None
        for i, g, d in ((ix, GX, o[0]), (iy, GY, o[1]), (iz, GZ, o[2])):
            d = d * sign
            if d:
                t = (i + d >= 0) & (i + d < g)
                ok = t if ok is None else ok & t
        return ok

    def remote(ex, o, src, dst):
        return pltpu.make_async_remote_copy(
            src_ref=src, dst_ref=dst, send_sem=ssem.at[ex], recv_sem=rsem.at[ex],
            device_id={"gx": ix + o[0], "gy": iy + o[1], "gz": iz + o[2]}, device_id_type=MESH,
        )

    def fine(ex, e, core):
        def make(k, far):
            o = a, b, c = OFFSETS[k]
            ys, yd, yn = cut(b, ny, H)
            if c == 0:
                if a == 0:
                    xs, xd, xn = 0, H, nx
                else:
                    lo, hi = (NEAR, FAR[e]) if far else (0, NEAR)
                    xs, xd, xn = (nx - hi, H - hi, hi - lo) if a > 0 else (lo, H + nx + lo, hi - lo)
                src = core.at[pl.ds(xs, xn), pl.ds(ys, yn)]
                dst = land.at[e, pl.ds(xd, xn), pl.ds(yd, yn)]
            else:
                f, side = (1, 0) if c > 0 else (0, 1)
                if a == 0:
                    src, dst = face.at[e, f, pl.ds(ys, yn)], edge.at[e, side, 1, pl.ds(yd, yn)]
                else:
                    src, dst = corner.at[e, (1 - a) // 2, f], cland.at[e, side, (1 - a) // 2, 1 - b]
            return ex + far, o, src, dst
        return make

    def level1(ex, e, h):
        def make(k, far):
            o = a, b, c = OFFSETS[k]
            xs, xd, xn = cut(a, n1x, h)
            ys, yd, yn = cut(b, n1y, H)
            if c == 0:
                src = send1.at[e, pl.ds(xs, xn), pl.ds(ys, yn)]
                dst = land1.at[e, pl.ds(xd, xn), pl.ds(yd, yn)]
            else:
                src, dst = face1.at[e, pl.ds(ys, yn)], edge1.at[e, 0 if c > 0 else 1, 1 - a, pl.ds(yd, yn)]
            return ex, o, src, dst
        return make

    FLAT = [k for k, o in enumerate(OFFSETS) if o[2] == 0]
    PACKED = [k for k, o in enumerate(OFFSETS) if o[2] != 0]
    WIDER = [k for k, o in enumerate(OFFSETS) if o[2] == 0 and o[0] != 0]
    sent = []

    def start(makers, ks, far=0):
        for k in ks:
            @pl.when(there(OFFSETS[k], 1))
            def _():
                for make in makers:
                    remote(*make(k, far)).start()

    def counts(i, g):
        if g < 3:
            return [(g - 1, None)]
        outer = (i == 0) | (i == g - 1)
        return [(1, outer), (2, jnp.logical_not(outer))]

    def settle(makers, ks, far, received):
        for cx, px in counts(ix, GX):
            for cy, py in counts(iy, GY):
                for cz, pz in counts(iz, GZ):
                    n = 0
                    for k in ks:
                        a, b, c = OFFSETS[k]
                        if min(a, b, c) >= 0:
                            times = (cx if a else 1) * (cy if b else 1) * (cz if c else 1)
                            for make in makers:
                                n += times * math.prod(make(k, far)[2].shape) // (H * LANES)
                    if n == 0:
                        continue
                    some = spare.at[pl.ds(0, n)]
                    copy = remote(makers[0](0, far)[0], (0, 0, 1), some, some)
                    wait = copy.wait_recv if received else copy.wait_send
                    ok = [p for p in (px, py, pz) if p is not None]
                    if ok:
                        pl.when(functools.reduce(jnp.logical_and, ok))(wait)
                    else:
                        wait()

    def finish(makers, ks, far=0):
        settle(makers, ks, far, True)
        sent.append((makers, ks, far))

    def drain():
        for makers, ks, far in sent:
            settle(makers, ks, far, False)

    def ends(k, sender):
        if k == 0:
            return etile, eslots.at[sender]
        if k < 3:
            return tile.at[k - 1], slots.at[k - 1, sender]
        return row.at[k - 3], rows.at[k - 3, sender]

    def gather_start(k):
        src, dst = ends(k, me)

        def body(d, _):
            pltpu.make_async_remote_copy(
                src_ref=src, dst_ref=dst, send_sem=gssem.at[k], recv_sem=grsem.at[k],
                device_id=device(me + d), device_id_type=MESH,
            ).start()
            return 0
        lax.fori_loop(1, N, body, 0)
        dst[...] = src[...]

    def everyone(k):
        some = pl.ds(0, N - 1)
        ref = eslots.at[some] if k == 0 else slots.at[k - 1, some] if k < 3 else rows.at[k - 3, some]
        return pltpu.make_async_remote_copy(
            src_ref=ref, dst_ref=ref, send_sem=gssem.at[k], recv_sem=grsem.at[k],
            device_id=device(me + 1), device_id_type=MESH,
        )

    def gather_finish(k):
        everyone(k).wait_recv()

    def gather_drain(k):
        everyone(k).wait_send()

    lane = iota((1, LANES), 1)

    def pack0(e, core):
        first = jnp.zeros((ny, LANES), F32)
        last = jnp.zeros((ny, LANES), F32)
        for x in range(nx):
            v = core[x]
            here = (lane >= H * x) & (lane < H * x + H)
            first = jnp.where(here, pltpu.roll(v, H * x, 1) if x else v, first)
            last = jnp.where(here, pltpu.roll(v, (H * x + H) % LANES, 1) if (H * x + H) % LANES else v, last)
        for f, v in enumerate((first, last)):
            face[e, f] = v
            for i, base in enumerate((nx - DEEP, 0)):
                fold = jnp.zeros((H, LANES), F32)
                for k in range(ny // H):
                    lo = H * DEEP * k
                    shift = (lo - H * base) % LANES
                    part = v[H * k : H * k + H]
                    part = pltpu.roll(part, shift, 1) if shift else part
                    fold = jnp.where((lane >= lo) & (lane < lo + H * DEEP), part, fold)
                corner[e, i, f] = fold

    def unfold(e):
        for side in range(2):
            for i in range(2):
                for k in range(-1, ny // H + 1):
                    v = cland[e, side, i, 0 if k < 0 else 2 if k == ny // H else 1]
                    shift = -H * DEEP * (k % (ny // H)) % LANES
                    edge[e, side, 2 * i, H * k + H : H * k + 2 * H] = pltpu.roll(v, shift, 1) if shift else v

    pl.semaphore_wait(barrier, N - 1)
    for load in loads:
        load.wait()
    both = [fine(0, 0, d_ref), fine(0, 1, x_ref)]
    start(both, FLAT)
    pack0(0, d_ref)
    pack0(1, x_ref)
    start(both, PACKED)
    start(both, WIDER, 1)

    def off0(l):
        return jnp.where(l < 192, l, l - 256)

    def off1(l):
        return jnp.where(l < 96, l, l - 128)

    def inside(v, i, n, g):
        v = v + i * n
        return (v >= 0) & (v < g * n)

    def f(cond, value=1.0):
        return jnp.where(cond, F32(value), F32(0.0))

    def near0(z):
        return (z >= -H) & (z < nz + H)

    def near1(z):
        return (z >= -H) & (z < n1z + H)

    yy, zz = iota((Y0, W0), 0) - H, off0(iota((Y0, W0), 1))
    M0[...] = f(inside(yy, iy, ny, GY) & inside(zz, iz, nz, GZ) & near0(zz))
    yy, zz = iota((Y1, LANES), 0) - H, off1(iota((Y1, LANES), 1))
    M1[...] = f(inside(yy, iy, n1y, GY) & inside(zz, iz, n1z, GZ) & near1(zz))
    everywhere = iota((1, LANES), 1)
    evens, halved = everywhere * 2 % LANES, everywhere // 2
    blocks = everywhere % n2z * 2
    MID = slice(H // 2, H // 2 + Y0 // 2)

    def put_halves(p, v):
        def store():
            S[0, p] = v[:, :LANES]
            S[1, p] = v[:, LANES:]
        return store

    def shrink0(p):
        def half(h):
            v = S[h, p, pl.ds(0, Y0 // 2, stride=2)] + S[h, p, pl.ds(1, Y0 // 2, stride=2)]
            return take(v + pltpu.roll(v, LANES - 1, 1), evens)
        return jnp.where(everywhere < n1z, half(0), half(1))

    def put_mid(ref, p, v):
        def store():
            ref[p, MID] = v
        return store

    def shrink1(src, p):
        v = src[p, pl.ds(H, n2y, stride=2)] + src[p, pl.ds(H + 1, n2y, stride=2)]
        return 0.5 * take(v + pltpu.roll(v, LANES - 1, 1), blocks)

    def xin0(p):
        return f(inside(p - H, ix, nx, GX))

    def xin1(p):
        return f(inside(p - H, ix, n1x, GX))

    def loop(lo, hi, body, group=1):
        count = hi - lo
        while count % group:
            group -= 1

        def step(i, _):
            stores = [body(lo + i * group + k) for k in range(group)]
            for store in stores:
                store()
            return 0
        if count == group:
            step(0, 0)
        else:
            lax.fori_loop(0, count // group, step, 0)

    def put(ref, p, v):
        def store():
            ref[p] = v
        return store

    def merged0(e, core, p, b, sx):
        right = pltpu.roll(edge[e, 1, b], (LANES - H * sx) % LANES, 1)
        left = pltpu.roll(edge[e, 0, b], (2 * LANES - H - H * sx) % LANES, 1)
        return land[e, p], jnp.where(lane < H, right, left)

    def merge0(e, core, emit, far=False):
        near = ((0, H - NEAR, H, DEEP - H), (1, H, H + nx, -H), (2, H + nx, H + nx + NEAR, -H - nx))
        rest = ((0, H - FAR[e], H - NEAR, DEEP - H), (2, H + nx + NEAR, H + nx + FAR[e], -H - nx))
        if not far:
            unfold(e)
            land[e, H : H + nx, H : H + ny] = core[...]
        for b, lo, hi, shift in rest if far else near:
            def body(p, b=b, shift=shift):
                t0, t1 = merged0(e, core, p, b, p + shift)
                ok = M0[...] * xin0(p) > 0.5
                return emit(p, jnp.where(ok, jnp.concatenate([t0, t1], axis=1), 0.0))
            loop(lo, hi, body, UM)

    none = jnp.zeros((2, Y1, LANES), F32)
    R1a[...] = jnp.zeros(R1a.shape, F32)
    D1[...] = jnp.zeros(D1.shape, F32)
    QP[...] = jnp.zeros(QP.shape, F32)

    def put_d(p, v):
        return put(D, p, v)

    def put_r(p, v):
        return put(R, p, v)

    finish(both, FLAT + PACKED)
    merge0(0, d_ref, put_d)
    merge0(1, x_ref, put_r)

    def pair_d(p):
        return put_halves(p, D[2 * p - H] + D[2 * p - H + 1])

    def make_d1(p):
        return put_mid(D1, p, 0.125 * shrink0(p))

    loop(H - 1, H + n1x + 1, pair_d, 5)
    loop(H - 1, H + n1x + 1, make_d1, 5)

    def pack1(e, src):
        edges = jnp.zeros((n1y, LANES), F32)
        for x in range(n1x):
            v = src[H + x, H : H + n1y]
            send1[e, x] = v
            lo = 2 * H * x
            low = pltpu.roll(v, lo, 1) if lo else v
            up = pltpu.roll(v, (lo + 2 * H - n1z) % LANES, 1) if (lo + 2 * H - n1z) % LANES else v
            edges = jnp.where((lane >= lo) & (lane < lo + H), low, edges)
            edges = jnp.where((lane >= lo + H) & (lane < lo + 2 * H), up, edges)
        face1[e] = edges

    def merge1(e, h, dst, inner=True):
        land1[e, H : H + n1x, H : H + n1y] = send1[e]
        for b, lo, hi, shift in (
            (0, H - h, H, n1x - H), (1, H, H + n1x, -H), (2, H + n1x, H + n1x + h, -H - n1x)
        ):
            if b == 1 and not inner:
                continue

            def body(p, b=b, shift=shift):
                sx = p + shift
                right = pltpu.roll(edge1[e, 1, b], (LANES + n1z - 2 * H * sx) % LANES, 1)
                left = pltpu.roll(edge1[e, 0, b], (2 * LANES - 2 * H - 2 * H * sx) % LANES, 1)
                v = jnp.where(lane < n1z, land1[e, p], jnp.where(lane < n1z + H, right, left))
                return put(dst, p, jnp.where(M1[...] * xin1(p) > 0.5, v, 0.0))
            loop(lo, hi, body, 5)

    pack1(2, D1)
    start([level1(6, 2, 4)], FLAT + PACKED)

    def coarsen(plane):
        total = jnp.zeros((n2y, LANES), F32)
        for x in range(n2x):
            T1[x] = plane(H + 2 * x) + plane(H + 2 * x + 1)
        for x in range(n2x):
            total = total + jnp.where((lane >= n2z * x) & (lane < n2z * x + n2z), shrink1(T1, x), 0.0)
        return total

    etile[...] = coarsen(lambda p: D1[p]) * 0.25
    gather_start(0)

    def block(src, q, at):
        shift = (n2z * (q - at)) % LANES
        return pltpu.roll(src, shift, 1) if shift else src

    def along(load, at):
        v = None
        for q in range(LANES // n2z):
            part = block(load(q), q, at)
            v = part if v is None else jnp.where(lane >= n2z * q, part, v)
        return v

    PER = LANES // n2z

    def spread(load, dst, ring):
        def body(a):
            for x in range(n2x):
                for b in range(GY):
                    for t in range(NZ2 // LANES):
                        v = along(lambda q: load((a * GY + b) * GZ + t * PER + q, 0), x)
                        dst[a * n2x + x + 2, n2y * b : n2y * b + n2y, LANES * t : LANES * t + LANES] = v
            return lambda: None
        loop(0, GX, body)
        if not ring:
            return

        def edges(a):
            for b in range(GY):
                for t in range(NZ2 // LANES):
                    for i, p in ((0, a * n2x + 1), (1, (a + 1) * n2x + 2)):
                        v = jnp.concatenate([
                            along(lambda q: load((a * GY + b) * GZ + t * PER + q, 1), i + h) for h in (0, 2)
                        ], axis=0)
                        at = (p, slice(n2y * b, n2y * b + n2y), slice(LANES * t, LANES * t + LANES))
                        dst[at] = dst[at] + v
            return lambda: None
        loop(0, GX, edges)
        zero = jnp.zeros((NY2, NZ2), F32)
        dst[1] = zero
        dst[NX2 + 2] = zero

    rows2, lanes2 = iota((NY2, NZ2), 0), iota((NY2, NZ2), 1)

    def box2(ref, p):
        s = ref[p - 1] + ref[p] + ref[p + 1]
        s = (
            s
            + jnp.where(rows2 > 0, pltpu.roll(s, 1, 0), 0.0)
            + jnp.where(rows2 < NY2 - 1, pltpu.roll(s, NY2 - 1, 0), 0.0)
        )
        return (
            s
            + jnp.where(lanes2 > 0, pltpu.roll(s, 1, 1), 0.0)
            + jnp.where(lanes2 < NZ2 - 1, pltpu.roll(s, NZ2 - 1, 1), 0.0)
        )

    zero2 = jnp.zeros((2, NY2, NZ2), F32)
    for ref in (G, Q, Y):
        ref[0:2] = zero2
        ref[NX2 + 2 : NX2 + 4] = zero2

    def coarse():
        theta, delta, sigma = cheb_terms(1.0)
        rho1 = 1.0 / sigma
        rho2 = 1.0 / (2.0 * sigma - rho1)
        rho3 = 1.0 / (2.0 * sigma - rho2)
        a2, b2 = rho2 * rho1, 2.0 * rho2 / delta
        a3, b3 = rho3 * rho2, 2.0 * rho3 / delta

        def first(p):
            g = G[p]
            remain = g - ((27.0 + E[p]) * g - box2(G, p)) * (1.0 / theta)
            a, b = put(Q, p, (a2 / theta) * g + b2 * remain), put(Y, p, remain)
            return lambda: (a(), b())

        def second(p):
            q, g = Q[p], G[p]
            remain = Y[p] - ((27.0 + E[p]) * q - box2(Q, p))
            return put(Y, p, (1.0 / theta) * g + (1.0 + a3) * q + b3 * remain)

        def third(p):
            y = Y[p]
            left = G[p] - ((27.0 + E[p]) * y - box2(Y, p))
            shift = jnp.sum(left, axis=1, keepdims=True) * lines[p][:, 0:1]

            def store():
                QP[p, H : H + NY2] = y + shift
            return store

        for body, reach in ((first, 4), (second, 3), (third, 2)):
            count = min(n2x + 2 * reach, NX2)
            base = jnp.clip(ix * n2x - reach, 0, NX2 - count) + 2
            loop(0, count, lambda p: body(base + p), UC)

    def line_sums():
        def body(p):
            v = 1.0 / jnp.sum(1.0 + E[p], axis=1, keepdims=True)
            return put(lines, p, jnp.broadcast_to(v, (NY2, LANES)))
        loop(2, NX2 + 2, body, UC)

    def smooth1(ref, p):
        return ref[p] * (k3 - k2 * D1[p]) + k2 * box(ref, p)

    def precondition(it):
        ex = 4 + it

        def down0(p):
            return put(Z, p, (M0[...] * xin0(p)) * (R[p] * (k3 - k2 * D[p]) + k2 * box(R, p)))

        loop(H - 1, H + nx + 1, down0, 6)

        def rest0(p):
            return R[p] - ((27.0 + D[p]) * Z[p] - box(Z, p))

        def pair0(p):
            return put_halves(p, rest0(2 * p - H) + rest0(2 * p - H + 1))

        def down1(p):
            return put_mid(R1a, p, 0.5 * M1[MID] * shrink0(p))

        loop(H, H + n1x, pair0, 2)
        loop(H, H + n1x, down1, 8)

        pack1(it, R1a)
        fine1 = [level1(ex, it, 5)]
        start(fine1, FLAT + PACKED)

        Z1[H - 3 : H - 1] = none
        Z1[H + n1x + 1 : H + n1x + 3] = none

        def z1a(p):
            return put(Z1, p, (M1[...] * xin1(p)) * smooth1(R1a, p))

        loop(H - 1, H + n1x + 1, z1a, 5)

        def rest1(p):
            return R1a[p] - ((27.0 + D1[p]) * Z1[p] - box(Z1, p))

        tile[it, 0:n2y] = coarsen(rest1)
        T1[n2x] = box(Z1, H - 2) + rest1(H - 1)
        T1[n2x + 1] = rest1(H + n1x) + box(Z1, H + n1x + 1)
        low, high = shrink1(T1, n2x), shrink1(T1, n2x + 1)
        low, high = (jnp.where(lane < 2 * n2z, v, pltpu.roll(v, n2y // 2, 0)) for v in (low, high))
        ring2 = jnp.where(lane // n2z % 2 == 0, low, high)
        tile[it, n2y : n2y + n2y // 2] = ring2[0 : n2y // 2]
        gather_start(1 + it)

        far(it)
        for lo, hi in ((H - 3, H - 1), (H + nx + 1, H + nx + 3)):
            loop(lo, hi, down0, 2)

        finish(fine1, FLAT + PACKED)
        merge1(it, 5, R1)
        if it == 0:
            finish([level1(6, 2, 4)], FLAT + PACKED)
            merge1(2, 4, D1, False)

        def z1b(p):
            return put(Z1, p, (M1[...] * xin1(p)) * smooth1(R1, p))

        loop(H - 4, H + n1x + 4, z1b, U1)

        if it == 0:
            gather_finish(0)
            spread(lambda n, r: eslots[n], E, False)
            line_sums()
        gather_finish(1 + it)
        spread(lambda n, r: slots[it, n, n2y:] if r else slots[it, n, 0:n2y], G, True)
        coarse()

        zz = off1(everywhere)
        source = (zz + iz * n1z) // 2
        fits = inside(zz, iz, n1z, GZ) & near1(zz)

        def wide1(q):
            rows2 = pl.ds(pl.multiple_of(iy * n2y, H), n2y + 2 * H)
            v = jnp.zeros((n1y, LANES), F32)
            for t in range(NZ2 // LANES):
                part = QP[ix * n2x + q, rows2, LANES * t : LANES * t + LANES][H // 2 : H // 2 + n1y]
                at = source - LANES * t
                v = jnp.where(fits & (at >= 0) & (at < LANES), take(part, jnp.clip(at, 0, LANES - 1)), v)

            def store():
                T1[q, pl.ds(0, n1y, stride=2)] = v
                T1[q, pl.ds(1, n1y, stride=2)] = v
            return store

        def up1(q):
            v = T1[q]
            p = H - 4 + 2 * q
            a, b = put(Z1, p, Z1[p] + v), put(Z1, p + 1, Z1[p + 1] + v)
            return lambda: (a(), b())

        loop(0, n2x + 4, wide1, 8)
        loop(0, n2x + 4, up1, 4)

        def t1(p):
            return put(T1, p, (M1[...] * xin1(p)) * (R1[p] - ((27.0 + D1[p]) * Z1[p] - box(Z1, p))))

        loop(H - 3, H + n1x + 3, t1, U1)

        def z1c(p):
            return put(Z1, p, Z1[p] + (M1[...] * xin1(p)) * smooth1(T1, p))

        loop(H - 2, H + n1x + 2, z1c, U1)

        def wide0(p):
            v = Z1[p, MID]
            parts = take(v, halved), take(v, halved + n1z)

            def store():
                for h, part in enumerate(parts):
                    S[h, p, pl.ds(0, Y0 // 2, stride=2)] = part
                    S[h, p, pl.ds(1, Y0 // 2, stride=2)] = part
            return store

        def up0(p):
            v = jnp.concatenate([S[0, p], S[1, p]], axis=1)
            q = 2 * p - H
            a, b = put(Z, q, Z[q] + v), put(Z, q + 1, Z[q + 1] + v)
            return lambda: (a(), b())

        loop(H - 2, H + n1x + 2, wide0, 4)
        loop(H - 2, H + n1x + 2, up0, 4)

        def t0(p):
            return put(T, p, (M0[...] * xin0(p)) * rest0(p))

        loop(H - 2, H + nx + 2, t0, UF)

        def z0(p):
            return put(Z, p, Z[p] + (M0[...] * xin0(p)) * (T[p] * (k3 - k2 * D[p]) + k2 * box(T, p)))

        loop(H - 1, H + nx + 1, z0, UF)

    core = (slice(H, H + ny), slice(0, nz))

    def products(it):
        def one(x, carry):
            p = x + H
            z = Z[p]
            w = ((27.0 + D[p]) * z - box(Z, p))[core[0], core[1]]
            z = z[core[0], core[1]]
            W[it, x] = w
            S0[it, x] = z
            r = R[p, core[0], core[1]]
            out = [carry[0] + r * z, carry[1] + z * w]
            if it:
                out.append(carry[2] + z * W[0, x])
            return tuple(out)

        def body(i, carry):
            for k in range(UP):
                carry = one(i * UP + k, carry)
            return carry

        init = tuple(jnp.zeros((ny, nz), F32) for _ in range(3 if it else 2))
        sums = lax.fori_loop(0, nx // UP, body, init)
        v = jnp.zeros((1, LANES), F32)
        for i, s in enumerate(sums):
            s = jnp.sum(jnp.sum(s, axis=0, keepdims=True), axis=1, keepdims=True)
            v = jnp.where(lane == i, s, v)
        row[it] = v
        gather_start(3 + it)

    def total(k):
        gather_finish(k)

        def body(n, acc):
            return acc + rows[k - 3, n]

        acc = lax.fori_loop(0, N, body, jnp.zeros((1, LANES), F32))
        return acc[:, 0:1], acc[:, 1:2], acc[:, 2:3]

    def far(it):
        if it == 0:
            finish(both, WIDER, 1)
            merge0(0, d_ref, put_d, True)
            merge0(1, x_ref, put_r, True)
        else:
            finish(image, WIDER, 1)
            merge0(2, W.at[0], put_image, True)

    precondition(0)
    products(0)
    image = [fine(2, 2, W.at[0])]
    start(image, FLAT)
    pack0(2, W.at[0])
    start(image, PACKED)
    start(image, WIDER, 1)
    rz0, curve0, _ = total(3)
    alpha0 = rz0 / curve0
    finish(image, FLAT + PACKED)

    def put_image(p, v):
        return put(R, p, R[p] - alpha0 * v)

    merge0(2, W.at[0], put_image)
    precondition(1)
    products(1)
    rz1, zw, zq = total(4)
    beta = rz1 / rz0
    curve = zw + 2.0 * beta * zq + beta * beta * curve0
    alpha = rz1 / curve

    def last(x):
        z = S0[0, x]
        sol_ref[x] = alpha0 * z + alpha * (S0[1, x] + beta * z)
        res_ref[x] = R[x + H, core[0], core[1]] - alpha * (W[1, x] + beta * W[0, x])
        return lambda: None

    loop(0, nx, last, 4)
    drain()
    for k in range(5):
        gather_drain(k)


def solution(mesh):
    dims = (mesh.shape["gx"], mesh.shape["gy"], mesh.shape["gz"])
    N = dims[0] * dims[1] * dims[2]

    def local(right_side, diagonal):
        nx, ny, nz = right_side.shape
        assert nz == LANES and nx * H == LANES and (nx // 4) * (nz // 4) == LANES and ny == 32
        n1x, n1y, n2y = nx // 2, ny // 2, ny // 4
        X0, Y0, X1, Y1 = nx + 2 * H, ny + 2 * H, n1x + 2 * H, n1y + 2 * H
        NX2, NY2, NZ2 = dims[0] * nx // 4, dims[1] * n2y, dims[2] * nz // 4
        W0 = 2 * LANES
        vm = lambda *s: pltpu.VMEM(s, F32)
        dma = pltpu.SemaphoreType.DMA
        scratch = [
            vm(nx, ny, nz), vm(nx, ny, nz),
            vm(3, X0, Y0, LANES), vm(3, 2, 3, Y0, LANES), vm(3, 2, ny, LANES),
            vm(3, 2, 2, H, LANES), vm(3, 2, 2, 3, H, LANES),
            vm(X0, Y0, W0), vm(X0, Y0, W0), vm(X0, Y0, W0), vm(X0, Y0, W0),
            vm(2, nx, ny, nz), vm(2, nx, ny, nz),
            vm(3, X1, Y1, LANES), vm(3, 2, 3, Y1, LANES), vm(3, n1y, LANES),
            vm(X1, Y1, LANES), vm(X1, Y1, LANES), vm(X1, Y1, LANES), vm(X1, Y1, LANES), vm(X1, Y1, LANES),
            vm(3, n1x, n1y, LANES),
            vm(2, N, n2y * 3 // 2, LANES), vm(2, n2y * 3 // 2, LANES), vm(N, n2y, LANES), vm(n2y, LANES), vm(2, N, 1, LANES), vm(2, 1, LANES),
            vm(NX2 + 4, NY2, NZ2), vm(NX2 + 4, NY2, NZ2), vm(NX2 + 4, NY2, NZ2), vm(NX2 + 4, NY2, NZ2),
            vm(NX2 + 4, NY2 + 2 * H, NZ2), vm(NX2 + 4, NY2, LANES), vm(2, X0, Y0, LANES), vm(Y0, W0), vm(Y1, LANES),
            vm(256, H, LANES), dma((7,)), dma((7,)), dma((5,)), dma((5,)), dma((2,)),
        ]
        shape = pltpu.VMEM(right_side.shape, F32)
        return pl.pallas_call(
            functools.partial(kernel, dims),
            out_shape=(shape, shape),
            in_specs=[pl.BlockSpec(memory_space=pl.ANY)] * 2,
            out_specs=[pl.BlockSpec(memory_space=pltpu.VMEM)] * 2,
            scratch_shapes=scratch,
            compiler_params=pltpu.CompilerParams(collective_id=0, has_side_effects=True),
        )(right_side, diagonal)

    placed = (P("gx", "gy", "gz"), P("gx", "gy", "gz"))
    return jax.shard_map(local, mesh=mesh, in_specs=placed, out_specs=placed, check_vma=False)
```

```python
import functools
import math

import jax
import jax.numpy as jnp
from jax import lax
from jax.experimental import pallas as pl
from jax.experimental.pallas import tpu as pltpu
from jax.sharding import PartitionSpec as P

ITERS = 2
LANES = 128
H = 8
MESH = pl.DeviceIdType.MESH
F32 = jnp.float32
UF, UR, U1, UC, UM, UP = 4, 8, 8, 12, 8, 4
OFFSETS = [
    (a, b, c) for a in (-1, 0, 1) for b in (-1, 0, 1) for c in (-1, 0, 1) if (a, b, c) != (0, 0, 0)
]
OFFSETS.sort(key=lambda o: (o[0] == 0, o[2] == 0, o[1] == 0))


def cheb_terms(lower):
    upper = 58.0
    theta = (upper + lower) / 2.0
    delta = (upper - lower) / 2.0
    return theta, delta, theta / delta


def cheb_two(lower):
    theta, delta, sigma = cheb_terms(lower)
    rho = 1.0 / sigma
    rho_next = 1.0 / (2.0 * sigma - rho)
    gain = 2.0 * rho_next / delta
    k2 = gain / theta
    k3 = (1.0 + rho_next * rho) / theta + gain - 27.0 * k2
    return k2, k3


def take(v, index):
    return jnp.take_along_axis(v, jnp.broadcast_to(index, v.shape), axis=1, mode="promise_in_bounds")


def iota(shape, dim):
    return lax.broadcasted_iota(jnp.int32, shape, dim)


def ring(s, rows, lanes):
    s = s + pltpu.roll(s, 1, 0) + pltpu.roll(s, rows - 1, 0)
    return s + pltpu.roll(s, 1, 1) + pltpu.roll(s, lanes - 1, 1)


def box(ref, p):
    s = ref[p - 1] + ref[p] + ref[p + 1]
    return ring(s, *s.shape)


def kernel(
    dims, x_hbm, d_hbm, sol_ref, res_ref,
    x_ref, d_ref, land, edge, face, corner, cland, D, R, Z, T, W, S0,
    land1, edge1, face1, D1, R1a, R1, Z1, T1, send1,
    slots, tile, eslots, etile, rows, row, G, E, Y, Q, QP, lines, S, M0, M1,
    spare, ssem, rsem, gssem, grsem, csem,
):
    GX, GY, GZ = dims
    N = GX * GY * GZ
    nx, ny, nz = x_ref.shape
    n1x, n1y, n1z = nx // 2, ny // 2, nz // 2
    n2x, n2y, n2z = nx // 4, ny // 4, nz // 4
    Y0, Y1 = ny + 2 * H, n1y + 2 * H
    NX2, NY2, NZ2 = GX * n2x, GY * n2y, GZ * n2z
    ix, iy, iz = lax.axis_index("gx"), lax.axis_index("gy"), lax.axis_index("gz")
    me = (ix * GY + iy) * GZ + iz
    k2, k3 = cheb_two(7.0)
    W0 = 2 * LANES

    FAR = (3, 4, 4)
    NEAR = 2
    DEEP = LANES // ny

    def device(n):
        n = lax.rem(n, N)
        return {"gx": lax.div(n, GY * GZ), "gy": lax.rem(lax.div(n, GZ), GY), "gz": lax.rem(n, GZ)}

    loads = [
        pltpu.make_async_copy(src, dst, csem.at[i])
        for i, (src, dst) in enumerate(((d_hbm, d_ref), (x_hbm, x_ref)))
    ]
    barrier = pltpu.get_barrier_semaphore()

    def greet(d, _):
        pl.semaphore_signal(barrier, inc=1, device_id=device(me + d), device_id_type=MESH)
        return 0

    lax.fori_loop(1, N, greet, 0)
    for load in loads:
        load.start()

    def cut(o, n, h):
        if o == 0:
            return 0, H, n
        if o > 0:
            return n - h, H - h, h
        return 0, H + n, h

    def there(o, sign):
        ok = None
        for i, g, d in ((ix, GX, o[0]), (iy, GY, o[1]), (iz, GZ, o[2])):
            d = d * sign
            if d:
                t = (i + d >= 0) & (i + d < g)
                ok = t if ok is None else ok & t
        return ok

    def remote(ex, o, src, dst):
        return pltpu.make_async_remote_copy(
            src_ref=src, dst_ref=dst, send_sem=ssem.at[ex], recv_sem=rsem.at[ex],
            device_id={"gx": ix + o[0], "gy": iy + o[1], "gz": iz + o[2]}, device_id_type=MESH,
        )

    def fine(ex, e, core):
        def make(k, far):
            o = a, b, c = OFFSETS[k]
            ys, yd, yn = cut(b, ny, H)
            if c == 0:
                if a == 0:
                    xs, xd, xn = 0, H, nx
                else:
                    lo, hi = (NEAR, FAR[e]) if far else (0, NEAR)
                    xs, xd, xn = (nx - hi, H - hi, hi - lo) if a > 0 else (lo, H + nx + lo, hi - lo)
                src = core.at[pl.ds(xs, xn), pl.ds(ys, yn)]
                dst = land.at[e, pl.ds(xd, xn), pl.ds(yd, yn)]
            else:
                f, side = (1, 0) if c > 0 else (0, 1)
                if a == 0:
                    src, dst = face.at[e, f, pl.ds(ys, yn)], edge.at[e, side, 1, pl.ds(yd, yn)]
                else:
                    src, dst = corner.at[e, (1 - a) // 2, f], cland.at[e, side, (1 - a) // 2, 1 - b]
            return ex + far, o, src, dst
        return make

    def level1(ex, e, h):
        def make(k, far):
            o = a, b, c = OFFSETS[k]
            xs, xd, xn = cut(a, n1x, h)
            ys, yd, yn = cut(b, n1y, H)
            if c == 0:
                src = send1.at[e, pl.ds(xs, xn), pl.ds(ys, yn)]
                dst = land1.at[e, pl.ds(xd, xn), pl.ds(yd, yn)]
            else:
                src, dst = face1.at[e, pl.ds(ys, yn)], edge1.at[e, 0 if c > 0 else 1, 1 - a, pl.ds(yd, yn)]
            return ex, o, src, dst
        return make

    FLAT = [k for k, o in enumerate(OFFSETS) if o[2] == 0]
    PACKED = [k for k, o in enumerate(OFFSETS) if o[2] != 0]
    WIDER = [k for k, o in enumerate(OFFSETS) if o[2] == 0 and o[0] != 0]
    sent = []

    def start(makers, ks, far=0):
        for k in ks:
            @pl.when(there(OFFSETS[k], 1))
            def _():
                for make in makers:
                    remote(*make(k, far)).start()

    def counts(i, g):
        if g < 3:
            return [(g - 1, None)]
        outer = (i == 0) | (i == g - 1)
        return [(1, outer), (2, jnp.logical_not(outer))]

    def settle(makers, ks, far, received):
        for cx, px in counts(ix, GX):
            for cy, py in counts(iy, GY):
                for cz, pz in counts(iz, GZ):
                    n = 0
                    for k in ks:
                        a, b, c = OFFSETS[k]
                        if min(a, b, c) >= 0:
                            times = (cx if a else 1) * (cy if b else 1) * (cz if c else 1)
                            for make in makers:
                                n += times * math.prod(make(k, far)[2].shape) // (H * LANES)
                    if n == 0:
                        continue
                    some = spare.at[pl.ds(0, n)]
                    copy = remote(makers[0](0, far)[0], (0, 0, 1), some, some)
                    wait = copy.wait_recv if received else copy.wait_send
                    ok = [p for p in (px, py, pz) if p is not None]
                    if ok:
                        pl.when(functools.reduce(jnp.logical_and, ok))(wait)
                    else:
                        wait()

    def finish(makers, ks, far=0):
        settle(makers, ks, far, True)
        sent.append((makers, ks, far))

    def drain():
        for makers, ks, far in sent:
            settle(makers, ks, far, False)

    def ends(k, sender):
        if k == 0:
            return etile, eslots.at[sender]
        if k < 3:
            return tile.at[k - 1], slots.at[k - 1, sender]
        return row.at[k - 3], rows.at[k - 3, sender]

    def gather_start(k):
        src, dst = ends(k, me)

        def body(d, _):
            pltpu.make_async_remote_copy(
                src_ref=src, dst_ref=dst, send_sem=gssem.at[k], recv_sem=grsem.at[k],
                device_id=device(me + d), device_id_type=MESH,
            ).start()
            return 0
        lax.fori_loop(1, N, body, 0)
        dst[...] = src[...]

    def everyone(k):
        some = pl.ds(0, N - 1)
        ref = eslots.at[some] if k == 0 else slots.at[k - 1, some] if k < 3 else rows.at[k - 3, some]
        return pltpu.make_async_remote_copy(
            src_ref=ref, dst_ref=ref, send_sem=gssem.at[k], recv_sem=grsem.at[k],
            device_id=device(me + 1), device_id_type=MESH,
        )

    def gather_finish(k):
        everyone(k).wait_recv()

    def gather_drain(k):
        everyone(k).wait_send()

    lane = iota((1, LANES), 1)

    def pack0(e, core):
        first = jnp.zeros((ny, LANES), F32)
        last = jnp.zeros((ny, LANES), F32)
        for x in range(nx):
            v = core[x]
            here = (lane >= H * x) & (lane < H * x + H)
            first = jnp.where(here, pltpu.roll(v, H * x, 1) if x else v, first)
            last = jnp.where(here, pltpu.roll(v, (H * x + H) % LANES, 1) if (H * x + H) % LANES else v, last)
        for f, v in enumerate((first, last)):
            face[e, f] = v
            for i, base in enumerate((nx - DEEP, 0)):
                fold = jnp.zeros((H, LANES), F32)
                for k in range(ny // H):
                    lo = H * DEEP * k
                    shift = (lo - H * base) % LANES
                    part = v[H * k : H * k + H]
                    part = pltpu.roll(part, shift, 1) if shift else part
                    fold = jnp.where((lane >= lo) & (lane < lo + H * DEEP), part, fold)
                corner[e, i, f] = fold

    def unfold(e):
        for side in range(2):
            for i in range(2):
                for k in range(-1, ny // H + 1):
                    v = cland[e, side, i, 0 if k < 0 else 2 if k == ny // H else 1]
                    shift = -H * DEEP * (k % (ny // H)) % LANES
                    edge[e, side, 2 * i, H * k + H : H * k + 2 * H] = pltpu.roll(v, shift, 1) if shift else v

    pl.semaphore_wait(barrier, N - 1)
    for load in loads:
        load.wait()
    both = [fine(0, 0, d_ref), fine(0, 1, x_ref)]
    start(both, FLAT)
    pack0(0, d_ref)
    pack0(1, x_ref)
    start(both, PACKED)
    start(both, WIDER, 1)

    def off0(l):
        return jnp.where(l < 192, l, l - 256)

    def off1(l):
        return jnp.where(l < 96, l, l - 128)

    def inside(v, i, n, g):
        v = v + i * n
        return (v >= 0) & (v < g * n)

    def f(cond, value=1.0):
        return jnp.where(cond, F32(value), F32(0.0))

    def near0(z):
        return (z >= -H) & (z < nz + H)

    def near1(z):
        return (z >= -H) & (z < n1z + H)

    yy, zz = iota((Y0, W0), 0) - H, off0(iota((Y0, W0), 1))
    M0[...] = f(inside(yy, iy, ny, GY) & inside(zz, iz, nz, GZ) & near0(zz))
    yy, zz = iota((Y1, LANES), 0) - H, off1(iota((Y1, LANES), 1))
    M1[...] = f(inside(yy, iy, n1y, GY) & inside(zz, iz, n1z, GZ) & near1(zz))
    everywhere = iota((1, LANES), 1)
    evens, halved = everywhere * 2 % LANES, everywhere // 2
    blocks = everywhere % n2z * 2
    MID = slice(H // 2, H // 2 + Y0 // 2)

    def put_halves(p, v):
        def store():
            S[0, p] = v[:, :LANES]
            S[1, p] = v[:, LANES:]
        return store

    def shrink0(p):
        def half(h):
            v = S[h, p, pl.ds(0, Y0 // 2, stride=2)] + S[h, p, pl.ds(1, Y0 // 2, stride=2)]
            return take(v + pltpu.roll(v, LANES - 1, 1), evens)
        return jnp.where(everywhere < n1z, half(0), half(1))

    def put_mid(ref, p, v):
        def store():
            ref[p, MID] = v
        return store

    def shrink1(src, p):
        v = src[p, pl.ds(H, n2y, stride=2)] + src[p, pl.ds(H + 1, n2y, stride=2)]
        return 0.5 * take(v + pltpu.roll(v, LANES - 1, 1), blocks)

    def xin0(p):
        return f(inside(p - H, ix, nx, GX))

    def xin1(p):
        return f(inside(p - H, ix, n1x, GX))

    def loop(lo, hi, body, group=1):
        count = hi - lo
        while count % group:
            group -= 1

        def step(i, _):
            stores = [body(lo + i * group + k) for k in range(group)]
            for store in stores:
                store()
            return 0
        if count == group:
            step(0, 0)
        else:
            lax.fori_loop(0, count // group, step, 0)

    def put(ref, p, v):
        def store():
            ref[p] = v
        return store

    def merged0(e, core, p, b, sx):
        right = pltpu.roll(edge[e, 1, b], (LANES - H * sx) % LANES, 1)
        left = pltpu.roll(edge[e, 0, b], (2 * LANES - H - H * sx) % LANES, 1)
        return land[e, p], jnp.where(lane < H, right, left)

    def merge0(e, core, emit, far=False):
        near = ((0, H - NEAR, H, DEEP - H), (1, H, H + nx, -H), (2, H + nx, H + nx + NEAR, -H - nx))
        rest = ((0, H - FAR[e], H - NEAR, DEEP - H), (2, H + nx + NEAR, H + nx + FAR[e], -H - nx))
        if not far:
            unfold(e)
            land[e, H : H + nx, H : H + ny] = core[...]
        for b, lo, hi, shift in rest if far else near:
            def body(p, b=b, shift=shift):
                t0, t1 = merged0(e, core, p, b, p + shift)
                ok = M0[...] * xin0(p) > 0.5
                return emit(p, jnp.where(ok, jnp.concatenate([t0, t1], axis=1), 0.0))
            loop(lo, hi, body, UM)

    none = jnp.zeros((2, Y1, LANES), F32)
    R1a[...] = jnp.zeros(R1a.shape, F32)
    D1[...] = jnp.zeros(D1.shape, F32)
    QP[...] = jnp.zeros(QP.shape, F32)

    def put_d(p, v):
        return put(D, p, v)

    def put_r(p, v):
        return put(R, p, v)

    finish(both, FLAT + PACKED)
    merge0(0, d_ref, put_d)
    merge0(1, x_ref, put_r)

    def pair_d(p):
        return put_halves(p, D[2 * p - H] + D[2 * p - H + 1])

    def make_d1(p):
        return put_mid(D1, p, 0.125 * shrink0(p))

    loop(H - 1, H + n1x + 1, pair_d, 5)
    loop(H - 1, H + n1x + 1, make_d1, 5)

    def pack1(e, src):
        edges = jnp.zeros((n1y, LANES), F32)
        for x in range(n1x):
            v = src[H + x, H : H + n1y]
            send1[e, x] = v
            lo = 2 * H * x
            low = pltpu.roll(v, lo, 1) if lo else v
            up = pltpu.roll(v, (lo + 2 * H - n1z) % LANES, 1) if (lo + 2 * H - n1z) % LANES else v
            edges = jnp.where((lane >= lo) & (lane < lo + H), low, edges)
            edges = jnp.where((lane >= lo + H) & (lane < lo + 2 * H), up, edges)
        face1[e] = edges

    def merge1(e, h, dst, inner=True):
        land1[e, H : H + n1x, H : H + n1y] = send1[e]
        for b, lo, hi, shift in (
            (0, H - h, H, n1x - H), (1, H, H + n1x, -H), (2, H + n1x, H + n1x + h, -H - n1x)
        ):
            if b == 1 and not inner:
                continue

            def body(p, b=b, shift=shift):
                sx = p + shift
                right = pltpu.roll(edge1[e, 1, b], (LANES + n1z - 2 * H * sx) % LANES, 1)
                left = pltpu.roll(edge1[e, 0, b], (2 * LANES - 2 * H - 2 * H * sx) % LANES, 1)
                v = jnp.where(lane < n1z, land1[e, p], jnp.where(lane < n1z + H, right, left))
                return put(dst, p, jnp.where(M1[...] * xin1(p) > 0.5, v, 0.0))
            loop(lo, hi, body, 5)

    pack1(2, D1)
    start([level1(6, 2, 4)], FLAT + PACKED)

    def coarsen(plane):
        total = jnp.zeros((n2y, LANES), F32)
        for x in range(n2x):
            T1[x] = plane(H + 2 * x) + plane(H + 2 * x + 1)
        for x in range(n2x):
            total = total + jnp.where((lane >= n2z * x) & (lane < n2z * x + n2z), shrink1(T1, x), 0.0)
        return total

    etile[...] = coarsen(lambda p: D1[p]) * 0.25
    gather_start(0)

    def block(src, q, at):
        shift = (n2z * (q - at)) % LANES
        return pltpu.roll(src, shift, 1) if shift else src

    def along(load, at):
        v = None
        for q in range(LANES // n2z):
            part = block(load(q), q, at)
            v = part if v is None else jnp.where(lane >= n2z * q, part, v)
        return v

    PER = LANES // n2z

    def spread(load, dst, ring):
        def body(a):
            for x in range(n2x):
                for b in range(GY):
                    for t in range(NZ2 // LANES):
                        v = along(lambda q: load((a * GY + b) * GZ + t * PER + q, 0), x)
                        dst[a * n2x + x + 2, n2y * b : n2y * b + n2y, LANES * t : LANES * t + LANES] = v
            return lambda: None
        loop(0, GX, body, GX)
        if not ring:
            return

        def edges(a):
            for b in range(GY):
                for t in range(NZ2 // LANES):
                    for i, p in ((0, a * n2x + 1), (1, (a + 1) * n2x + 2)):
                        v = jnp.concatenate([
                            along(lambda q: load((a * GY + b) * GZ + t * PER + q, 1), i + h) for h in (0, 2)
                        ], axis=0)
                        at = (p, slice(n2y * b, n2y * b + n2y), slice(LANES * t, LANES * t + LANES))
                        dst[at] = dst[at] + v
            return lambda: None
        loop(0, GX, edges, GX)
        zero = jnp.zeros((NY2, NZ2), F32)
        dst[1] = zero
        dst[NX2 + 2] = zero

    rows2, lanes2 = iota((NY2, NZ2), 0), iota((NY2, NZ2), 1)

    def box2(ref, p):
        s = ref[p - 1] + ref[p] + ref[p + 1]
        s = (
            s
            + jnp.where(rows2 > 0, pltpu.roll(s, 1, 0), 0.0)
            + jnp.where(rows2 < NY2 - 1, pltpu.roll(s, NY2 - 1, 0), 0.0)
        )
        return (
            s
            + jnp.where(lanes2 > 0, pltpu.roll(s, 1, 1), 0.0)
            + jnp.where(lanes2 < NZ2 - 1, pltpu.roll(s, NZ2 - 1, 1), 0.0)
        )

    zero2 = jnp.zeros((2, NY2, NZ2), F32)
    for ref in (G, Q, Y):
        ref[0:2] = zero2
        ref[NX2 + 2 : NX2 + 4] = zero2

    def coarse():
        theta, delta, sigma = cheb_terms(1.0)
        rho1 = 1.0 / sigma
        rho2 = 1.0 / (2.0 * sigma - rho1)
        rho3 = 1.0 / (2.0 * sigma - rho2)
        a2, b2 = rho2 * rho1, 2.0 * rho2 / delta
        a3, b3 = rho3 * rho2, 2.0 * rho3 / delta

        def first(p):
            g = G[p]
            remain = g - ((27.0 + E[p]) * g - box2(G, p)) * (1.0 / theta)
            a, b = put(Q, p, (a2 / theta) * g + b2 * remain), put(Y, p, remain)
            return lambda: (a(), b())

        def second(p):
            q, g = Q[p], G[p]
            remain = Y[p] - ((27.0 + E[p]) * q - box2(Q, p))
            return put(Y, p, (1.0 / theta) * g + (1.0 + a3) * q + b3 * remain)

        def third(p):
            y = Y[p]
            left = G[p] - ((27.0 + E[p]) * y - box2(Y, p))
            shift = jnp.sum(left, axis=1, keepdims=True) * lines[p][:, 0:1]

            def store():
                QP[p, H : H + NY2] = y + shift
            return store

        for body, reach in ((first, 4), (second, 3), (third, 2)):
            count = min(n2x + 2 * reach, NX2)
            base = jnp.clip(ix * n2x - reach, 0, NX2 - count) + 2
            loop(0, count, lambda p: body(base + p), UC)

    def line_sums():
        def body(p):
            v = 1.0 / jnp.sum(1.0 + E[p], axis=1, keepdims=True)
            return put(lines, p, jnp.broadcast_to(v, (NY2, LANES)))
        loop(2, NX2 + 2, body, UC)

    def smooth1(ref, p):
        return ref[p] * (k3 - k2 * D1[p]) + k2 * box(ref, p)

    def precondition(it):
        ex = 4 + it

        def down0(p):
            return put(Z, p, (M0[...] * xin0(p)) * (R[p] * (k3 - k2 * D[p]) + k2 * box(R, p)))

        loop(H - 1, H + nx + 1, down0, 6)

        def rest0(p):
            return R[p] - ((27.0 + D[p]) * Z[p] - box(Z, p))

        def pair0(p):
            return put_halves(p, rest0(2 * p - H) + rest0(2 * p - H + 1))

        def down1(p):
            return put_mid(R1a, p, 0.5 * M1[MID] * shrink0(p))

        loop(H, H + n1x, pair0, 4)
        loop(H, H + n1x, down1, 8)

        pack1(it, R1a)
        fine1 = [level1(ex, it, 5)]

        Z1[H - 3 : H - 1] = none
        Z1[H + n1x + 1 : H + n1x + 3] = none

        def z1a(p):
            return put(Z1, p, (M1[...] * xin1(p)) * smooth1(R1a, p))

        loop(H - 1, H + n1x + 1, z1a, 5)

        def rest1(p):
            return R1a[p] - ((27.0 + D1[p]) * Z1[p] - box(Z1, p))

        tile[it, 0:n2y] = coarsen(rest1)
        T1[n2x] = box(Z1, H - 2) + rest1(H - 1)
        T1[n2x + 1] = rest1(H + n1x) + box(Z1, H + n1x + 1)
        low, high = shrink1(T1, n2x), shrink1(T1, n2x + 1)
        low, high = (jnp.where(lane < 2 * n2z, v, pltpu.roll(v, n2y // 2, 0)) for v in (low, high))
        ring2 = jnp.where(lane // n2z % 2 == 0, low, high)
        tile[it, n2y : n2y + n2y // 2] = ring2[0 : n2y // 2]
        gather_start(1 + it)
        start(fine1, FLAT + PACKED)

        far(it)
        for lo, hi in ((H - 3, H - 1), (H + nx + 1, H + nx + 3)):
            loop(lo, hi, down0, 2)

        if it == 0:
            gather_finish(0)
            spread(lambda n, r: eslots[n], E, False)
            line_sums()
        gather_finish(1 + it)
        spread(lambda n, r: slots[it, n, n2y:] if r else slots[it, n, 0:n2y], G, True)
        coarse()
        finish(fine1, FLAT + PACKED)
        merge1(it, 5, R1)
        if it == 0:
            finish([level1(6, 2, 4)], FLAT + PACKED)
            merge1(2, 4, D1, False)

        def z1b(p):
            return put(Z1, p, (M1[...] * xin1(p)) * smooth1(R1, p))

        loop(H - 4, H + n1x + 4, z1b, U1)


        zz = off1(everywhere)
        source = (zz + iz * n1z) // 2
        fits = inside(zz, iz, n1z, GZ) & near1(zz)

        def wide1(q):
            rows2 = pl.ds(pl.multiple_of(iy * n2y, H), n2y + 2 * H)
            v = jnp.zeros((n1y, LANES), F32)
            for t in range(NZ2 // LANES):
                part = QP[ix * n2x + q, rows2, LANES * t : LANES * t + LANES][H // 2 : H // 2 + n1y]
                at = source - LANES * t
                v = jnp.where(fits & (at >= 0) & (at < LANES), take(part, jnp.clip(at, 0, LANES - 1)), v)

            def store():
                T1[q, pl.ds(0, n1y, stride=2)] = v
                T1[q, pl.ds(1, n1y, stride=2)] = v
            return store

        def up1(q):
            v = T1[q]
            p = H - 4 + 2 * q
            a, b = put(Z1, p, Z1[p] + v), put(Z1, p + 1, Z1[p + 1] + v)
            return lambda: (a(), b())

        loop(0, n2x + 4, wide1, 8)
        loop(0, n2x + 4, up1, 8)

        def t1(p):
            return put(T1, p, (M1[...] * xin1(p)) * (R1[p] - ((27.0 + D1[p]) * Z1[p] - box(Z1, p))))

        loop(H - 3, H + n1x + 3, t1, 7)

        def z1c(p):
            return put(Z1, p, Z1[p] + (M1[...] * xin1(p)) * smooth1(T1, p))

        loop(H - 2, H + n1x + 2, z1c, 6)

        def wide0(p):
            v = Z1[p, MID]
            parts = take(v, halved), take(v, halved + n1z)

            def store():
                for h, part in enumerate(parts):
                    S[h, p, pl.ds(0, Y0 // 2, stride=2)] = part
                    S[h, p, pl.ds(1, Y0 // 2, stride=2)] = part
            return store

        def up0(p):
            v = jnp.concatenate([S[0, p], S[1, p]], axis=1)
            q = 2 * p - H
            a, b = put(Z, q, Z[q] + v), put(Z, q + 1, Z[q + 1] + v)
            return lambda: (a(), b())

        loop(H - 2, H + n1x + 2, wide0, 12)
        loop(H - 2, H + n1x + 2, up0, 6)

        def t0(p):
            return put(T, p, (M0[...] * xin0(p)) * rest0(p))

        loop(H - 2, H + nx + 2, t0, 5)

        def z0(p):
            return put(Z, p, Z[p] + (M0[...] * xin0(p)) * (T[p] * (k3 - k2 * D[p]) + k2 * box(T, p)))

        loop(H - 1, H + nx + 1, z0, 6)

    core = (slice(H, H + ny), slice(0, nz))

    def products(it):
        def one(x, carry):
            p = x + H
            z = Z[p]
            w = ((27.0 + D[p]) * z - box(Z, p))[core[0], core[1]]
            z = z[core[0], core[1]]
            W[it, x] = w
            S0[it, x] = z
            r = R[p, core[0], core[1]]
            out = [carry[0] + r * z, carry[1] + z * w]
            if it:
                out.append(carry[2] + z * W[0, x])
            return tuple(out)

        def body(i, carry):
            for k in range(UP):
                carry = one(i * UP + k, carry)
            return carry

        init = tuple(jnp.zeros((ny, nz), F32) for _ in range(3 if it else 2))
        sums = lax.fori_loop(0, nx // UP, body, init)
        v = jnp.zeros((1, LANES), F32)
        for i, s in enumerate(sums):
            s = jnp.sum(jnp.sum(s, axis=0, keepdims=True), axis=1, keepdims=True)
            v = jnp.where(lane == i, s, v)
        row[it] = v
        gather_start(3 + it)

    def total(k):
        gather_finish(k)

        def body(n, acc):
            return acc + rows[k - 3, n]

        acc = lax.fori_loop(0, N, body, jnp.zeros((1, LANES), F32))
        return acc[:, 0:1], acc[:, 1:2], acc[:, 2:3]

    def far(it):
        if it == 0:
            finish(both, WIDER, 1)
            merge0(0, d_ref, put_d, True)
            merge0(1, x_ref, put_r, True)
        else:
            finish(image, WIDER, 1)
            merge0(2, W.at[0], put_image, True)

    precondition(0)
    products(0)
    image = [fine(2, 2, W.at[0])]
    start(image, FLAT)
    pack0(2, W.at[0])
    start(image, PACKED)
    start(image, WIDER, 1)
    rz0, curve0, _ = total(3)
    alpha0 = rz0 / curve0
    finish(image, FLAT + PACKED)

    def put_image(p, v):
        return put(R, p, R[p] - alpha0 * v)

    merge0(2, W.at[0], put_image)
    precondition(1)
    products(1)
    rz1, zw, zq = total(4)
    beta = rz1 / rz0
    curve = zw + 2.0 * beta * zq + beta * beta * curve0
    alpha = rz1 / curve

    def last(x):
        z = S0[0, x]
        sol_ref[x] = alpha0 * z + alpha * (S0[1, x] + beta * z)
        res_ref[x] = R[x + H, core[0], core[1]] - alpha * (W[1, x] + beta * W[0, x])
        return lambda: None

    loop(0, nx, last, 4)
    drain()
    for k in range(5):
        gather_drain(k)


def solution(mesh):
    dims = (mesh.shape["gx"], mesh.shape["gy"], mesh.shape["gz"])
    N = dims[0] * dims[1] * dims[2]

    def local(right_side, diagonal):
        nx, ny, nz = right_side.shape
        assert nz == LANES and nx * H == LANES and (nx // 4) * (nz // 4) == LANES and ny == 32
        n1x, n1y, n2y = nx // 2, ny // 2, ny // 4
        X0, Y0, X1, Y1 = nx + 2 * H, ny + 2 * H, n1x + 2 * H, n1y + 2 * H
        NX2, NY2, NZ2 = dims[0] * nx // 4, dims[1] * n2y, dims[2] * nz // 4
        W0 = 2 * LANES
        vm = lambda *s: pltpu.VMEM(s, F32)
        dma = pltpu.SemaphoreType.DMA
        scratch = [
            vm(nx, ny, nz), vm(nx, ny, nz),
            vm(3, X0, Y0, LANES), vm(3, 2, 3, Y0, LANES), vm(3, 2, ny, LANES),
            vm(3, 2, 2, H, LANES), vm(3, 2, 2, 3, H, LANES),
            vm(X0, Y0, W0), vm(X0, Y0, W0), vm(X0, Y0, W0), vm(X0, Y0, W0),
            vm(2, nx, ny, nz), vm(2, nx, ny, nz),
            vm(3, X1, Y1, LANES), vm(3, 2, 3, Y1, LANES), vm(3, n1y, LANES),
            vm(X1, Y1, LANES), vm(X1, Y1, LANES), vm(X1, Y1, LANES), vm(X1, Y1, LANES), vm(X1, Y1, LANES),
            vm(3, n1x, n1y, LANES),
            vm(2, N, n2y * 3 // 2, LANES), vm(2, n2y * 3 // 2, LANES), vm(N, n2y, LANES), vm(n2y, LANES), vm(2, N, 1, LANES), vm(2, 1, LANES),
            vm(NX2 + 4, NY2, NZ2), vm(NX2 + 4, NY2, NZ2), vm(NX2 + 4, NY2, NZ2), vm(NX2 + 4, NY2, NZ2),
            vm(NX2 + 4, NY2 + 2 * H, NZ2), vm(NX2 + 4, NY2, LANES), vm(2, X0, Y0, LANES), vm(Y0, W0), vm(Y1, LANES),
            vm(256, H, LANES), dma((7,)), dma((7,)), dma((5,)), dma((5,)), dma((2,)),
        ]
        shape = pltpu.VMEM(right_side.shape, F32)
        return pl.pallas_call(
            functools.partial(kernel, dims),
            out_shape=(shape, shape),
            in_specs=[pl.BlockSpec(memory_space=pl.ANY)] * 2,
            out_specs=[pl.BlockSpec(memory_space=pltpu.VMEM)] * 2,
            scratch_shapes=scratch,
            compiler_params=pltpu.CompilerParams(collective_id=0, has_side_effects=True),
        )(right_side, diagonal)

    placed = (P("gx", "gy", "gz"), P("gx", "gy", "gz"))
    return jax.shard_map(local, mesh=mesh, in_specs=placed, out_specs=placed, check_vma=False)
```

```python
import functools
import math

import jax
import jax.numpy as jnp
from jax import lax
from jax.experimental import pallas as pl
from jax.experimental.pallas import tpu as pltpu
from jax.sharding import PartitionSpec as P

ITERS = 2
LANES = 128
H = 8
MESH = pl.DeviceIdType.MESH
F32 = jnp.float32
UF, UR, U1, UC, UM, UP = 4, 8, 8, 12, 8, 4
OFFSETS = [
    (a, b, c) for a in (-1, 0, 1) for b in (-1, 0, 1) for c in (-1, 0, 1) if (a, b, c) != (0, 0, 0)
]
OFFSETS.sort(key=lambda o: (o[0] == 0, o[2] == 0, o[1] == 0))


def cheb_terms(lower):
    upper = 58.0
    theta = (upper + lower) / 2.0
    delta = (upper - lower) / 2.0
    return theta, delta, theta / delta


def cheb_two(lower):
    theta, delta, sigma = cheb_terms(lower)
    rho = 1.0 / sigma
    rho_next = 1.0 / (2.0 * sigma - rho)
    gain = 2.0 * rho_next / delta
    k2 = gain / theta
    k3 = (1.0 + rho_next * rho) / theta + gain - 27.0 * k2
    return k2, k3


def take(v, index):
    return jnp.take_along_axis(v, jnp.broadcast_to(index, v.shape), axis=1, mode="promise_in_bounds")


def iota(shape, dim):
    return lax.broadcasted_iota(jnp.int32, shape, dim)


def ring(s, rows, lanes):
    s = s + pltpu.roll(s, 1, 0) + pltpu.roll(s, rows - 1, 0)
    return s + pltpu.roll(s, 1, 1) + pltpu.roll(s, lanes - 1, 1)


def box(ref, p):
    s = ref[p - 1] + ref[p] + ref[p + 1]
    return ring(s, *s.shape)


def kernel(
    dims, x_hbm, d_hbm, sol_ref, res_ref,
    x_ref, d_ref, land, edge, face, corner, cland, D, R, Z, T, W, S0,
    land1, edge1, face1, D1, R1a, R1, Z1, T1, send1,
    slots, tile, eslots, etile, rows, row, G, E, Y, Q, QP, lines, S, M0, M1,
    spare, ssem, rsem, gssem, grsem, csem,
):
    GX, GY, GZ = dims
    N = GX * GY * GZ
    nx, ny, nz = x_ref.shape
    n1x, n1y, n1z = nx // 2, ny // 2, nz // 2
    n2x, n2y, n2z = nx // 4, ny // 4, nz // 4
    Y0, Y1 = ny + 2 * H, n1y + 2 * H
    NX2, NY2, NZ2 = GX * n2x, GY * n2y, GZ * n2z
    ix, iy, iz = lax.axis_index("gx"), lax.axis_index("gy"), lax.axis_index("gz")
    me = (ix * GY + iy) * GZ + iz
    k2, k3 = cheb_two(7.0)
    W0 = 2 * LANES

    FAR = (3, 4, 4)
    NEAR = 2
    DEEP = LANES // ny

    def device(n):
        n = lax.rem(n, N)
        return {"gx": lax.div(n, GY * GZ), "gy": lax.rem(lax.div(n, GZ), GY), "gz": lax.rem(n, GZ)}

    loads = [
        pltpu.make_async_copy(src, dst, csem.at[i])
        for i, (src, dst) in enumerate(((d_hbm, d_ref), (x_hbm, x_ref)))
    ]
    barrier = pltpu.get_barrier_semaphore()

    def greet(d, _):
        pl.semaphore_signal(barrier, inc=1, device_id=device(me + d), device_id_type=MESH)
        return 0

    lax.fori_loop(1, N, greet, 0)
    for load in loads:
        load.start()

    def cut(o, n, h):
        if o == 0:
            return 0, H, n
        if o > 0:
            return n - h, H - h, h
        return 0, H + n, h

    def there(o, sign):
        ok = None
        for i, g, d in ((ix, GX, o[0]), (iy, GY, o[1]), (iz, GZ, o[2])):
            d = d * sign
            if d:
                t = (i + d >= 0) & (i + d < g)
                ok = t if ok is None else ok & t
        return ok

    def remote(ex, o, src, dst):
        return pltpu.make_async_remote_copy(
            src_ref=src, dst_ref=dst, send_sem=ssem.at[ex], recv_sem=rsem.at[ex],
            device_id={"gx": ix + o[0], "gy": iy + o[1], "gz": iz + o[2]}, device_id_type=MESH,
        )

    def fine(ex, e, core):
        def make(k, far):
            o = a, b, c = OFFSETS[k]
            ys, yd, yn = cut(b, ny, H)
            if c == 0:
                if a == 0:
                    xs, xd, xn = 0, H, nx
                else:
                    lo, hi = (NEAR, FAR[e]) if far else (0, NEAR)
                    xs, xd, xn = (nx - hi, H - hi, hi - lo) if a > 0 else (lo, H + nx + lo, hi - lo)
                src = core.at[pl.ds(xs, xn), pl.ds(ys, yn)]
                dst = land.at[e, pl.ds(xd, xn), pl.ds(yd, yn)]
            else:
                f, side = (1, 0) if c > 0 else (0, 1)
                if a == 0:
                    src, dst = face.at[e, f, pl.ds(ys, yn)], edge.at[e, side, 1, pl.ds(yd, yn)]
                else:
                    src, dst = corner.at[e, (1 - a) // 2, f], cland.at[e, side, (1 - a) // 2, 1 - b]
            return ex + far, o, src, dst
        return make

    def level1(ex, e, h):
        def make(k, far):
            o = a, b, c = OFFSETS[k]
            xs, xd, xn = cut(a, n1x, h)
            ys, yd, yn = cut(b, n1y, H)
            if c == 0:
                src = send1.at[e, pl.ds(xs, xn), pl.ds(ys, yn)]
                dst = land1.at[e, pl.ds(xd, xn), pl.ds(yd, yn)]
            else:
                src, dst = face1.at[e, pl.ds(ys, yn)], edge1.at[e, 0 if c > 0 else 1, 1 - a, pl.ds(yd, yn)]
            return ex, o, src, dst
        return make

    FLAT = [k for k, o in enumerate(OFFSETS) if o[2] == 0]
    PACKED = [k for k, o in enumerate(OFFSETS) if o[2] != 0]
    WIDER = [k for k, o in enumerate(OFFSETS) if o[2] == 0 and o[0] != 0]
    sent = []

    def start(makers, ks, far=0):
        for k in ks:
            @pl.when(there(OFFSETS[k], 1))
            def _():
                for make in makers:
                    remote(*make(k, far)).start()

    def counts(i, g):
        if g < 3:
            return [(g - 1, None)]
        outer = (i == 0) | (i == g - 1)
        return [(1, outer), (2, jnp.logical_not(outer))]

    def settle(makers, ks, far, received):
        for cx, px in counts(ix, GX):
            for cy, py in counts(iy, GY):
                for cz, pz in counts(iz, GZ):
                    n = 0
                    for k in ks:
                        a, b, c = OFFSETS[k]
                        if min(a, b, c) >= 0:
                            times = (cx if a else 1) * (cy if b else 1) * (cz if c else 1)
                            for make in makers:
                                n += times * math.prod(make(k, far)[2].shape) // (H * LANES)
                    if n == 0:
                        continue
                    some = spare.at[pl.ds(0, n)]
                    copy = remote(makers[0](0, far)[0], (0, 0, 1), some, some)
                    wait = copy.wait_recv if received else copy.wait_send
                    ok = [p for p in (px, py, pz) if p is not None]
                    if ok:
                        pl.when(functools.reduce(jnp.logical_and, ok))(wait)
                    else:
                        wait()

    def finish(makers, ks, far=0):
        settle(makers, ks, far, True)
        sent.append((makers, ks, far))

    def drain():
        for makers, ks, far in sent:
            settle(makers, ks, far, False)

    def ends(k, sender):
        if k == 0:
            return etile, eslots.at[sender]
        if k < 3:
            return tile.at[k - 1], slots.at[k - 1, sender]
        return row.at[k - 3], rows.at[k - 3, sender]

    def gather_start(k):
        src, dst = ends(k, me)

        def body(d, _):
            pltpu.make_async_remote_copy(
                src_ref=src, dst_ref=dst, send_sem=gssem.at[k], recv_sem=grsem.at[k],
                device_id=device(me + d), device_id_type=MESH,
            ).start()
            return 0
        lax.fori_loop(1, N, body, 0)
        dst[...] = src[...]

    def everyone(k):
        some = pl.ds(0, N - 1)
        ref = eslots.at[some] if k == 0 else slots.at[k - 1, some] if k < 3 else rows.at[k - 3, some]
        return pltpu.make_async_remote_copy(
            src_ref=ref, dst_ref=ref, send_sem=gssem.at[k], recv_sem=grsem.at[k],
            device_id=device(me + 1), device_id_type=MESH,
        )

    def gather_finish(k):
        everyone(k).wait_recv()

    def gather_drain(k):
        everyone(k).wait_send()

    lane = iota((1, LANES), 1)

    def pack0(e, core):
        first = jnp.zeros((ny, LANES), F32)
        last = jnp.zeros((ny, LANES), F32)
        for x in range(nx):
            v = core[x]
            here = (lane >= H * x) & (lane < H * x + H)
            first = jnp.where(here, pltpu.roll(v, H * x, 1) if x else v, first)
            last = jnp.where(here, pltpu.roll(v, (H * x + H) % LANES, 1) if (H * x + H) % LANES else v, last)
        for f, v in enumerate((first, last)):
            face[e, f] = v
            for i, base in enumerate((nx - DEEP, 0)):
                fold = jnp.zeros((H, LANES), F32)
                for k in range(ny // H):
                    lo = H * DEEP * k
                    shift = (lo - H * base) % LANES
                    part = v[H * k : H * k + H]
                    part = pltpu.roll(part, shift, 1) if shift else part
                    fold = jnp.where((lane >= lo) & (lane < lo + H * DEEP), part, fold)
                corner[e, i, f] = fold

    def unfold(e):
        for side in range(2):
            for i in range(2):
                for k in range(-1, ny // H + 1):
                    v = cland[e, side, i, 0 if k < 0 else 2 if k == ny // H else 1]
                    shift = -H * DEEP * (k % (ny // H)) % LANES
                    edge[e, side, 2 * i, H * k + H : H * k + 2 * H] = pltpu.roll(v, shift, 1) if shift else v

    pl.semaphore_wait(barrier, N - 1)
    for load in loads:
        load.wait()
    both = [fine(0, 0, d_ref), fine(0, 1, x_ref)]
    start(both, FLAT)
    pack0(0, d_ref)
    pack0(1, x_ref)
    start(both, PACKED)
    start(both, WIDER, 1)

    def off0(l):
        return jnp.where(l < 192, l, l - 256)

    def off1(l):
        return jnp.where(l < 96, l, l - 128)

    def inside(v, i, n, g):
        v = v + i * n
        return (v >= 0) & (v < g * n)

    def f(cond, value=1.0):
        return jnp.where(cond, F32(value), F32(0.0))

    def near0(z):
        return (z >= -H) & (z < nz + H)

    def near1(z):
        return (z >= -H) & (z < n1z + H)

    yy, zz = iota((Y0, W0), 0) - H, off0(iota((Y0, W0), 1))
    M0[...] = f(inside(yy, iy, ny, GY) & inside(zz, iz, nz, GZ) & near0(zz))
    yy, zz = iota((Y1, LANES), 0) - H, off1(iota((Y1, LANES), 1))
    M1[...] = f(inside(yy, iy, n1y, GY) & inside(zz, iz, n1z, GZ) & near1(zz))
    everywhere = iota((1, LANES), 1)
    evens, halved = everywhere * 2 % LANES, everywhere // 2
    blocks = everywhere % n2z * 2
    MID = slice(H // 2, H // 2 + Y0 // 2)

    def put_halves(p, v):
        def store():
            S[0, p] = v[:, :LANES]
            S[1, p] = v[:, LANES:]
        return store

    def shrink0(p):
        def half(h):
            v = S[h, p, pl.ds(0, Y0 // 2, stride=2)] + S[h, p, pl.ds(1, Y0 // 2, stride=2)]
            return take(v + pltpu.roll(v, LANES - 1, 1), evens)
        return jnp.where(everywhere < n1z, half(0), half(1))

    def put_mid(ref, p, v):
        def store():
            ref[p, MID] = v
        return store

    def shrink1(src, p):
        v = src[p, pl.ds(H, n2y, stride=2)] + src[p, pl.ds(H + 1, n2y, stride=2)]
        return 0.5 * take(v + pltpu.roll(v, LANES - 1, 1), blocks)

    def xin0(p):
        return f(inside(p - H, ix, nx, GX))

    def xin1(p):
        return f(inside(p - H, ix, n1x, GX))

    def loop(lo, hi, body, group=1):
        count = hi - lo
        while count % group:
            group -= 1

        def step(i, _):
            stores = [body(lo + i * group + k) for k in range(group)]
            for store in stores:
                store()
            return 0
        if count == group:
            step(0, 0)
        else:
            lax.fori_loop(0, count // group, step, 0)

    def put(ref, p, v):
        def store():
            ref[p] = v
        return store

    def merged0(e, core, p, b, sx):
        right = pltpu.roll(edge[e, 1, b], (LANES - H * sx) % LANES, 1)
        left = pltpu.roll(edge[e, 0, b], (2 * LANES - H - H * sx) % LANES, 1)
        return land[e, p], jnp.where(lane < H, right, left)

    def merge0(e, core, emit, far=False):
        near = ((0, H - NEAR, H, DEEP - H), (1, H, H + nx, -H), (2, H + nx, H + nx + NEAR, -H - nx))
        rest = ((0, H - FAR[e], H - NEAR, DEEP - H), (2, H + nx + NEAR, H + nx + FAR[e], -H - nx))
        if not far:
            unfold(e)
            land[e, H : H + nx, H : H + ny] = core[...]
        for b, lo, hi, shift in rest if far else near:
            def body(p, b=b, shift=shift):
                t0, t1 = merged0(e, core, p, b, p + shift)
                ok = M0[...] * xin0(p) > 0.5
                return emit(p, jnp.where(ok, jnp.concatenate([t0, t1], axis=1), 0.0))
            loop(lo, hi, body, UM)

    none = jnp.zeros((2, Y1, LANES), F32)
    R1a[...] = jnp.zeros(R1a.shape, F32)
    D1[...] = jnp.zeros(D1.shape, F32)
    QP[...] = jnp.zeros(QP.shape, F32)

    def put_d(p, v):
        return put(D, p, v)

    def put_r(p, v):
        return put(R, p, v)

    finish(both, FLAT + PACKED)
    merge0(0, d_ref, put_d)
    merge0(1, x_ref, put_r)

    def pair_d(p):
        return put_halves(p, D[2 * p - H] + D[2 * p - H + 1])

    def make_d1(p):
        return put_mid(D1, p, 0.125 * shrink0(p))

    loop(H - 1, H + n1x + 1, pair_d, 5)
    loop(H - 1, H + n1x + 1, make_d1, 5)

    def pack1(e, src):
        edges = jnp.zeros((n1y, LANES), F32)
        for x in range(n1x):
            v = src[H + x, H : H + n1y]
            send1[e, x] = v
            lo = 2 * H * x
            low = pltpu.roll(v, lo, 1) if lo else v
            up = pltpu.roll(v, (lo + 2 * H - n1z) % LANES, 1) if (lo + 2 * H - n1z) % LANES else v
            edges = jnp.where((lane >= lo) & (lane < lo + H), low, edges)
            edges = jnp.where((lane >= lo + H) & (lane < lo + 2 * H), up, edges)
        face1[e] = edges

    def merge1(e, h, dst, inner=True):
        land1[e, H : H + n1x, H : H + n1y] = send1[e]
        for b, lo, hi, shift in (
            (0, H - h, H, n1x - H), (1, H, H + n1x, -H), (2, H + n1x, H + n1x + h, -H - n1x)
        ):
            if b == 1 and not inner:
                continue

            def body(p, b=b, shift=shift):
                sx = p + shift
                right = pltpu.roll(edge1[e, 1, b], (LANES + n1z - 2 * H * sx) % LANES, 1)
                left = pltpu.roll(edge1[e, 0, b], (2 * LANES - 2 * H - 2 * H * sx) % LANES, 1)
                v = jnp.where(lane < n1z, land1[e, p], jnp.where(lane < n1z + H, right, left))
                return put(dst, p, jnp.where(M1[...] * xin1(p) > 0.5, v, 0.0))
            loop(lo, hi, body, 5)

    pack1(2, D1)
    start([level1(6, 2, 4)], FLAT + PACKED)

    def coarsen(plane):
        total = jnp.zeros((n2y, LANES), F32)
        for x in range(n2x):
            T1[x] = plane(H + 2 * x) + plane(H + 2 * x + 1)
        for x in range(n2x):
            total = total + jnp.where((lane >= n2z * x) & (lane < n2z * x + n2z), shrink1(T1, x), 0.0)
        return total

    etile[...] = coarsen(lambda p: D1[p]) * 0.25
    gather_start(0)

    def block(src, q, at):
        shift = (n2z * (q - at)) % LANES
        return pltpu.roll(src, shift, 1) if shift else src

    def along(load, at):
        v = None
        for q in range(LANES // n2z):
            part = block(load(q), q, at)
            v = part if v is None else jnp.where(lane >= n2z * q, part, v)
        return v

    PER = LANES // n2z

    def spread(load, dst, ring):
        def body(a):
            for x in range(n2x):
                for b in range(GY):
                    for t in range(NZ2 // LANES):
                        v = along(lambda q: load((a * GY + b) * GZ + t * PER + q, 0), x)
                        dst[a * n2x + x + 2, n2y * b : n2y * b + n2y, LANES * t : LANES * t + LANES] = v
            return lambda: None
        loop(0, GX, body, GX)
        if not ring:
            return

        def edges(a):
            for b in range(GY):
                for t in range(NZ2 // LANES):
                    for i, p in ((0, a * n2x + 1), (1, (a + 1) * n2x + 2)):
                        v = jnp.concatenate([
                            along(lambda q: load((a * GY + b) * GZ + t * PER + q, 1), i + h) for h in (0, 2)
                        ], axis=0)
                        at = (p, slice(n2y * b, n2y * b + n2y), slice(LANES * t, LANES * t + LANES))
                        dst[at] = dst[at] + v
            return lambda: None
        loop(0, GX, edges, GX)
        zero = jnp.zeros((NY2, NZ2), F32)
        dst[1] = zero
        dst[NX2 + 2] = zero

    rows2, lanes2 = iota((NY2, NZ2), 0), iota((NY2, NZ2), 1)

    def box2(ref, p):
        s = ref[p - 1] + ref[p] + ref[p + 1]
        s = (
            s
            + jnp.where(rows2 > 0, pltpu.roll(s, 1, 0), 0.0)
            + jnp.where(rows2 < NY2 - 1, pltpu.roll(s, NY2 - 1, 0), 0.0)
        )
        return (
            s
            + jnp.where(lanes2 > 0, pltpu.roll(s, 1, 1), 0.0)
            + jnp.where(lanes2 < NZ2 - 1, pltpu.roll(s, NZ2 - 1, 1), 0.0)
        )

    zero2 = jnp.zeros((2, NY2, NZ2), F32)
    for ref in (G, Q, Y):
        ref[0:2] = zero2
        ref[NX2 + 2 : NX2 + 4] = zero2

    def coarse():
        theta, delta, sigma = cheb_terms(1.0)
        rho1 = 1.0 / sigma
        rho2 = 1.0 / (2.0 * sigma - rho1)
        rho3 = 1.0 / (2.0 * sigma - rho2)
        a2, b2 = rho2 * rho1, 2.0 * rho2 / delta
        a3, b3 = rho3 * rho2, 2.0 * rho3 / delta

        def first(p):
            g = G[p]
            remain = g - ((27.0 + E[p]) * g - box2(G, p)) * (1.0 / theta)
            a, b = put(Q, p, (a2 / theta) * g + b2 * remain), put(Y, p, remain)
            return lambda: (a(), b())

        def second(p):
            q, g = Q[p], G[p]
            remain = Y[p] - ((27.0 + E[p]) * q - box2(Q, p))
            return put(Y, p, (1.0 / theta) * g + (1.0 + a3) * q + b3 * remain)

        def third(p):
            y = Y[p]
            left = G[p] - ((27.0 + E[p]) * y - box2(Y, p))
            shift = jnp.sum(left, axis=1, keepdims=True) * lines[p][:, 0:1]

            def store():
                QP[p, H : H + NY2] = y + shift
            return store

        for body, reach in ((first, 4), (second, 3), (third, 2)):
            count = min(n2x + 2 * reach, NX2)
            base = jnp.clip(ix * n2x - reach, 0, NX2 - count) + 2
            loop(0, count, lambda p: body(base + p), UC)

    def line_sums():
        def body(p):
            v = 1.0 / jnp.sum(1.0 + E[p], axis=1, keepdims=True)
            return put(lines, p, jnp.broadcast_to(v, (NY2, LANES)))
        loop(2, NX2 + 2, body, UC)

    def smooth1(ref, p):
        return ref[p] * (k3 - k2 * D1[p]) + k2 * box(ref, p)

    def precondition(it):
        ex = 4 + it

        def down0(p):
            return put(Z, p, (M0[...] * xin0(p)) * (R[p] * (k3 - k2 * D[p]) + k2 * box(R, p)))

        loop(H - 1, H + nx + 1, down0, 9)

        def rest0(p):
            return R[p] - ((27.0 + D[p]) * Z[p] - box(Z, p))

        def pair0(p):
            return put_halves(p, rest0(2 * p - H) + rest0(2 * p - H + 1))

        def down1(p):
            return put_mid(R1a, p, 0.5 * M1[MID] * shrink0(p))

        loop(H, H + n1x, pair0, 8)
        loop(H, H + n1x, down1, 8)

        fine1 = [level1(ex, it, 5)]

        Z1[H - 3 : H - 1] = none
        Z1[H + n1x + 1 : H + n1x + 3] = none

        def z1a(p):
            return put(Z1, p, (M1[...] * xin1(p)) * smooth1(R1a, p))

        loop(H - 1, H + n1x + 1, z1a, 5)

        def rest1(p):
            return R1a[p] - ((27.0 + D1[p]) * Z1[p] - box(Z1, p))

        tile[it, 0:n2y] = coarsen(rest1)
        T1[n2x] = box(Z1, H - 2) + rest1(H - 1)
        T1[n2x + 1] = rest1(H + n1x) + box(Z1, H + n1x + 1)
        low, high = shrink1(T1, n2x), shrink1(T1, n2x + 1)
        low, high = (jnp.where(lane < 2 * n2z, v, pltpu.roll(v, n2y // 2, 0)) for v in (low, high))
        ring2 = jnp.where(lane // n2z % 2 == 0, low, high)
        tile[it, n2y : n2y + n2y // 2] = ring2[0 : n2y // 2]
        gather_start(1 + it)
        pack1(it, R1a)
        start(fine1, FLAT + PACKED)

        far(it)
        for lo, hi in ((H - 3, H - 1), (H + nx + 1, H + nx + 3)):
            loop(lo, hi, down0, 2)

        if it == 0:
            gather_finish(0)
            spread(lambda n, r: eslots[n], E, False)
            line_sums()
        gather_finish(1 + it)
        spread(lambda n, r: slots[it, n, n2y:] if r else slots[it, n, 0:n2y], G, True)
        coarse()
        finish(fine1, FLAT + PACKED)
        merge1(it, 5, R1)
        if it == 0:
            finish([level1(6, 2, 4)], FLAT + PACKED)
            merge1(2, 4, D1, False)

        def z1b(p):
            return put(Z1, p, (M1[...] * xin1(p)) * smooth1(R1, p))

        loop(H - 4, H + n1x + 4, z1b, U1)


        zz = off1(everywhere)
        source = (zz + iz * n1z) // 2
        fits = inside(zz, iz, n1z, GZ) & near1(zz)

        def wide1(q):
            rows2 = pl.ds(pl.multiple_of(iy * n2y, H), n2y + 2 * H)
            v = jnp.zeros((n1y, LANES), F32)
            for t in range(NZ2 // LANES):
                part = QP[ix * n2x + q, rows2, LANES * t : LANES * t + LANES][H // 2 : H // 2 + n1y]
                at = source - LANES * t
                v = jnp.where(fits & (at >= 0) & (at < LANES), take(part, jnp.clip(at, 0, LANES - 1)), v)

            def store():
                T1[q, pl.ds(0, n1y, stride=2)] = v
                T1[q, pl.ds(1, n1y, stride=2)] = v
            return store

        def up1(q):
            v = T1[q]
            p = H - 4 + 2 * q
            a, b = put(Z1, p, Z1[p] + v), put(Z1, p + 1, Z1[p + 1] + v)
            return lambda: (a(), b())

        loop(0, n2x + 4, wide1, 8)
        loop(0, n2x + 4, up1, 8)

        def t1(p):
            return put(T1, p, (M1[...] * xin1(p)) * (R1[p] - ((27.0 + D1[p]) * Z1[p] - box(Z1, p))))

        loop(H - 3, H + n1x + 3, t1, 7)

        def z1c(p):
            return put(Z1, p, Z1[p] + (M1[...] * xin1(p)) * smooth1(T1, p))

        loop(H - 2, H + n1x + 2, z1c, 6)

        def wide0(p):
            v = Z1[p, MID]
            parts = take(v, halved), take(v, halved + n1z)

            def store():
                for h, part in enumerate(parts):
                    S[h, p, pl.ds(0, Y0 // 2, stride=2)] = part
                    S[h, p, pl.ds(1, Y0 // 2, stride=2)] = part
            return store

        def up0(p):
            v = jnp.concatenate([S[0, p], S[1, p]], axis=1)
            q = 2 * p - H
            a, b = put(Z, q, Z[q] + v), put(Z, q + 1, Z[q + 1] + v)
            return lambda: (a(), b())

        loop(H - 2, H + n1x + 2, wide0, 12)
        loop(H - 2, H + n1x + 2, up0, 6)

        def t0(p):
            return put(T, p, (M0[...] * xin0(p)) * rest0(p))

        loop(H - 2, H + nx + 2, t0, 10)

        def z0(p):
            return put(Z, p, Z[p] + (M0[...] * xin0(p)) * (T[p] * (k3 - k2 * D[p]) + k2 * box(T, p)))

        loop(H - 1, H + nx + 1, z0, 9)

    core = (slice(H, H + ny), slice(0, nz))

    def products(it):
        def one(x, carry):
            p = x + H
            z = Z[p]
            w = ((27.0 + D[p]) * z - box(Z, p))[core[0], core[1]]
            z = z[core[0], core[1]]
            W[it, x] = w
            S0[it, x] = z
            r = R[p, core[0], core[1]]
            out = [carry[0] + r * z, carry[1] + z * w]
            if it:
                out.append(carry[2] + z * W[0, x])
            return tuple(out)

        def body(i, carry):
            for k in range(UP):
                carry = one(i * UP + k, carry)
            return carry

        init = tuple(jnp.zeros((ny, nz), F32) for _ in range(3 if it else 2))
        sums = lax.fori_loop(0, nx // UP, body, init)
        v = jnp.zeros((1, LANES), F32)
        for i, s in enumerate(sums):
            s = jnp.sum(jnp.sum(s, axis=0, keepdims=True), axis=1, keepdims=True)
            v = jnp.where(lane == i, s, v)
        row[it] = v
        gather_start(3 + it)

    def total(k):
        gather_finish(k)

        def body(n, acc):
            return acc + rows[k - 3, n]

        acc = lax.fori_loop(0, N, body, jnp.zeros((1, LANES), F32))
        return acc[:, 0:1], acc[:, 1:2], acc[:, 2:3]

    def far(it):
        if it == 0:
            finish(both, WIDER, 1)
            merge0(0, d_ref, put_d, True)
            merge0(1, x_ref, put_r, True)
        else:
            finish(image, WIDER, 1)
            merge0(2, W.at[0], put_image, True)

    precondition(0)
    products(0)
    image = [fine(2, 2, W.at[0])]
    start(image, FLAT)
    pack0(2, W.at[0])
    start(image, PACKED)
    start(image, WIDER, 1)
    rz0, curve0, _ = total(3)
    alpha0 = rz0 / curve0
    finish(image, FLAT + PACKED)

    def put_image(p, v):
        return put(R, p, R[p] - alpha0 * v)

    merge0(2, W.at[0], put_image)
    precondition(1)
    products(1)
    rz1, zw, zq = total(4)
    beta = rz1 / rz0
    curve = zw + 2.0 * beta * zq + beta * beta * curve0
    alpha = rz1 / curve

    def last(x):
        z = S0[0, x]
        sol_ref[x] = alpha0 * z + alpha * (S0[1, x] + beta * z)
        res_ref[x] = R[x + H, core[0], core[1]] - alpha * (W[1, x] + beta * W[0, x])
        return lambda: None

    loop(0, nx, last, 4)
    drain()
    for k in range(5):
        gather_drain(k)


def solution(mesh):
    dims = (mesh.shape["gx"], mesh.shape["gy"], mesh.shape["gz"])
    N = dims[0] * dims[1] * dims[2]

    def local(right_side, diagonal):
        nx, ny, nz = right_side.shape
        assert nz == LANES and nx * H == LANES and (nx // 4) * (nz // 4) == LANES and ny == 32
        n1x, n1y, n2y = nx // 2, ny // 2, ny // 4
        X0, Y0, X1, Y1 = nx + 2 * H, ny + 2 * H, n1x + 2 * H, n1y + 2 * H
        NX2, NY2, NZ2 = dims[0] * nx // 4, dims[1] * n2y, dims[2] * nz // 4
        W0 = 2 * LANES
        vm = lambda *s: pltpu.VMEM(s, F32)
        dma = pltpu.SemaphoreType.DMA
        scratch = [
            vm(nx, ny, nz), vm(nx, ny, nz),
            vm(3, X0, Y0, LANES), vm(3, 2, 3, Y0, LANES), vm(3, 2, ny, LANES),
            vm(3, 2, 2, H, LANES), vm(3, 2, 2, 3, H, LANES),
            vm(X0, Y0, W0), vm(X0, Y0, W0), vm(X0, Y0, W0), vm(X0, Y0, W0),
            vm(2, nx, ny, nz), vm(2, nx, ny, nz),
            vm(3, X1, Y1, LANES), vm(3, 2, 3, Y1, LANES), vm(3, n1y, LANES),
            vm(X1, Y1, LANES), vm(X1, Y1, LANES), vm(X1, Y1, LANES), vm(X1, Y1, LANES), vm(X1, Y1, LANES),
            vm(3, n1x, n1y, LANES),
            vm(2, N, n2y * 3 // 2, LANES), vm(2, n2y * 3 // 2, LANES), vm(N, n2y, LANES), vm(n2y, LANES), vm(2, N, 1, LANES), vm(2, 1, LANES),
            vm(NX2 + 4, NY2, NZ2), vm(NX2 + 4, NY2, NZ2), vm(NX2 + 4, NY2, NZ2), vm(NX2 + 4, NY2, NZ2),
            vm(NX2 + 4, NY2 + 2 * H, NZ2), vm(NX2 + 4, NY2, LANES), vm(2, X0, Y0, LANES), vm(Y0, W0), vm(Y1, LANES),
            vm(256, H, LANES), dma((7,)), dma((7,)), dma((5,)), dma((5,)), dma((2,)),
        ]
        shape = pltpu.VMEM(right_side.shape, F32)
        return pl.pallas_call(
            functools.partial(kernel, dims),
            out_shape=(shape, shape),
            in_specs=[pl.BlockSpec(memory_space=pl.ANY)] * 2,
            out_specs=[pl.BlockSpec(memory_space=pltpu.VMEM)] * 2,
            scratch_shapes=scratch,
            compiler_params=pltpu.CompilerParams(collective_id=0, has_side_effects=True),
        )(right_side, diagonal)

    placed = (P("gx", "gy", "gz"), P("gx", "gy", "gz"))
    return jax.shard_map(local, mesh=mesh, in_specs=placed, out_specs=placed, check_vma=False)
```
